512 devices in a mesh: row: 32 (over y, x), col: 16 (over z, core).
Axes of the slice: x: 4, y: 8, z: 8, core: 2. Of those that a mesh axis runs over, the one named last changes fastest.
Arguments:
- ancestor: float32 [9, 9, 128, 2048], P(None, None, 'row', 'col'), may hold values from -1 to 4, as said below
- inverse_first: float32 [2, 2, 128, 2048], P(None, None, 'row', 'col'), may hold values from -1 to 2, as said below
- panel_first: float32 [1536, 2, 512], P('row', None, 'col'), may hold values from -0.15625 to 0.15625
- structure_first: int32 [1536], replicated, may hold values from 0 to 4607, as said below
- inverse_second: float32 [1, 1, 128, 2048], P(None, None, 'row', 'col'), may hold values from -1 to 2, as said below
- panel_second: float32 [1536, 1, 512], P('row', None, 'col'), may hold values from -0.15625 to 0.15625
- structure_second: int32 [1536], replicated, may hold values from 0 to 5631, as said below
Outputs:
- row_first: float32 [2, 11, 128, 2048], P(None, None, 'row', 'col')
- row_second: float32 [1, 12, 128, 2048], P(None, None, 'row', 'col')
The draws below stay inside these ranges and needn't reach their ends.
Inputs may be any that keep to these rules, and one draw needn't show every extreme that they name: `ancestor`: symmetric and positive definite as a matrix. `inverse_first`: symmetric and positive definite as a matrix. `inverse_second`: symmetric and positive definite as a matrix. `structure_first`: entries are distinct; every aligned group of 16 ancestor rows holds at most 6 entries, and some group holds exactly 6. `structure_second`: entries are distinct; every aligned group of 16 ancestor rows holds at most 6 entries, and some group holds exactly 6.
All inputs are finite; a program needn't handle non-finite values.
Results may differ from the reference program's by a relative error of at most 0.000075.
Values sent between devices are 32-bit elements; how exact they have to be, the bound alone decides.
No kernel may reach another device: no remote copies, remote signals or barrier semaphores. Data moves between devices by JAX's collectives and lax.ppermute only.
A program may use at most 64 MiB of HBM per device.

```python
import jax
import jax.numpy as jnp
from jax import lax

ANC = 4608
WA = 1024
WB = 512
NSA = 1536
NSB = 1536
TILE = 512
GRAIN = 16
CAP = 6
RH = 16
CW = 32


def pack_tiles(tiled):
    first, second = (tiled.shape[0], tiled.shape[1])
    grid_rows = TILE // RH
    grid_cols = TILE // CW
    depth = RH * CW // 128
    blocks = tiled.reshape(first, second, grid_rows, RH, grid_cols, CW).transpose(0, 1, 2, 4, 3, 5)
    blocks = blocks.reshape(first, second, grid_rows, grid_cols, depth, 128).transpose(0, 1, 2, 4, 3, 5)
    return blocks.reshape(first, second, grid_rows * depth, grid_cols * 128)


def definite_tiles(key, row_count, floor_level, ceiling_level, spread):
    first, second = jax.random.split(key)
    noise_field = jax.random.normal(first, (row_count, row_count), jnp.float32)
    levels = jax.random.uniform(second, (row_count,), jnp.float32, floor_level, ceiling_level)
    symmetric = (noise_field + noise_field.T) * (spread / jnp.sqrt(2.0 * row_count))
    matrix = symmetric + jnp.diag(levels)
    tile_count = row_count // TILE
    return pack_tiles(matrix.reshape(tile_count, TILE, tile_count, TILE).transpose(0, 2, 1, 3))


def grouped_structure(key, row_count, entry_count):
    group_count = row_count // GRAIN
    slot_count = group_count * CAP
    first_key, second_key, third_key = jax.random.split(key, 3)
    shuffled = jax.random.permutation(first_key, slot_count).astype(jnp.int32)
    forced = jax.random.randint(second_key, (), 0, group_count).astype(jnp.int32)
    slot_group = jnp.arange(slot_count, dtype=jnp.int32) // CAP
    ranking = jnp.where(slot_group == forced, shuffled - slot_count, shuffled)
    chosen = jnp.argsort(ranking, stable=True)[:entry_count].astype(jnp.int32)
    group_keys = jax.random.split(third_key, group_count)
    offsets = jax.vmap(lambda single: jax.random.permutation(single, GRAIN)[:CAP].astype(jnp.int32))(group_keys)
    group_of = chosen // CAP
    row_ids = group_of * GRAIN + offsets[group_of, chosen % CAP]
    return row_ids.astype(jnp.int32)


def draw_ancestor(key, part):
    return definite_tiles(jax.random.fold_in(key, 11), ANC, 1.5, 3.0, 0.7)


def draw_inverse_first(key, part):
    return definite_tiles(jax.random.fold_in(key, 12), WA, 0.8, 1.5, 0.3)


def draw_inverse_second(key, part):
    return definite_tiles(jax.random.fold_in(key, 13), WB, 0.8, 1.5, 0.3)


def draw_structure_first(key, part):
    return grouped_structure(jax.random.fold_in(key, 21), ANC, NSA)


def draw_structure_second(key, part):
    return grouped_structure(jax.random.fold_in(key, 22), ANC + WA, NSB)


def shard_levels(own_key, shape, cuts, low, high):
    level = 1.0
    for dim, parts in cuts:
        steps = jax.random.uniform(jax.random.fold_in(jax.random.fold_in(own_key, 6), dim), (parts,), jnp.float32, low / len(cuts), high / len(cuts))
        level = level * jnp.repeat(jnp.exp(steps), shape[dim] // parts).reshape((-1,) + (1,) * (len(shape) - 1 - dim))
    return level


def gaussian(rng, dims, scale, limit, shards=(), held_as=jnp.bfloat16):
    array = scale * jax.random.normal(rng, dims, jnp.float32)
    if shards:
        array = array * shard_levels(rng, dims, shards, -0.22, 0.18)
    return jnp.clip(array, -limit, limit).astype(held_as)


def setup_inputs(seed: int = 0) -> dict:
    arg_keys = jax.random.split(jax.random.key(seed), 8)
    return {
        "ancestor": draw_ancestor(jax.random.fold_in(arg_keys[7], 71), 0),
        "inverse_first": draw_inverse_first(jax.random.fold_in(arg_keys[7], 71), 0),
        "panel_first": gaussian(arg_keys[2], (NSA, WA // TILE, TILE), NSA ** -0.5, 0.15625, ((0, 32), (2, 16)), jnp.float32),
        "structure_first": draw_structure_first(jax.random.fold_in(arg_keys[7], 71), 0),
        "inverse_second": draw_inverse_second(jax.random.fold_in(arg_keys[7], 71), 0),
        "panel_second": gaussian(arg_keys[5], (NSB, WB // TILE, TILE), NSB ** -0.5, 0.15625, ((0, 32), (2, 16)), jnp.float32),
        "structure_second": draw_structure_second(jax.random.fold_in(arg_keys[7], 71), 0),
    }


def unpack(packed):
    first, second = packed.shape[0], packed.shape[1]
    grid_rows = TILE // RH
    grid_cols = TILE // CW
    depth = RH * CW // 128
    blocks = packed.reshape(first, second, grid_rows, depth, grid_cols, 128).transpose(0, 1, 2, 4, 3, 5)
    blocks = blocks.reshape(first, second, grid_rows, grid_cols, RH, CW).transpose(0, 1, 2, 4, 3, 5)
    return blocks.reshape(first, second, TILE, TILE)


def pack(tiled):
    first, second = tiled.shape[0], tiled.shape[1]
    grid_rows = TILE // RH
    grid_cols = TILE // CW
    depth = RH * CW // 128
    blocks = tiled.reshape(first, second, grid_rows, RH, grid_cols, CW).transpose(0, 1, 2, 4, 3, 5)
    blocks = blocks.reshape(first, second, grid_rows, grid_cols, depth, 128).transpose(0, 1, 2, 4, 3, 5)
    return blocks.reshape(first, second, grid_rows * depth, grid_cols * 128)


def from_tiles(packed):
    tiled = unpack(packed)
    first, second, height, width = tiled.shape
    return tiled.transpose(0, 2, 1, 3).reshape(first * height, second * width)


def to_tiles(matrix):
    first = matrix.shape[0] // TILE
    second = matrix.shape[1] // TILE
    return pack(matrix.reshape(first, TILE, second, TILE).transpose(0, 2, 1, 3))


def sweep_step(frontier, inverse, panel_part, structure):
    flattened = panel_part.reshape(panel_part.shape[0], -1)
    spread = jnp.zeros((frontier.shape[0], flattened.shape[1]), jnp.float32).at[structure].set(flattened)
    image = jnp.dot(frontier, spread, precision=lax.Precision.HIGHEST, preferred_element_type=jnp.float32)
    diagonal = from_tiles(inverse) + jnp.dot(spread.T, image, precision=lax.Precision.HIGHEST, preferred_element_type=jnp.float32)
    row_block = jnp.concatenate([-image.T, diagonal], axis=1)
    upper_rows = jnp.concatenate([frontier, -image], axis=1)
    grown = jnp.concatenate([upper_rows, row_block], axis=0)
    return row_block, grown


def reference(ancestor, inverse_first, panel_first, structure_first, inverse_second, panel_second, structure_second):
    first_block, frontier = sweep_step(from_tiles(ancestor), inverse_first, panel_first, structure_first)
    second_block, unused = sweep_step(frontier, inverse_second, panel_second, structure_second)
    return to_tiles(first_block), to_tiles(second_block)
```

```python
import jax
import jax.numpy as jnp
import numpy as np
from jax import lax
from jax.experimental import pallas as pl
from jax.experimental.pallas import tpu as pltpu
from jax.sharding import PartitionSpec as P

F32 = jnp.float32
BF16 = jnp.bfloat16
LINES = 40
TALL = 4 * LINES
SLOTS = 128
EXT = 16 * 2 * SLOTS

Y_GROUPS = [[4 * y + x for y in range(8)] for x in range(4)]
X_GROUPS = [[4 * y + x for x in range(4)] for y in range(8)]
Z_GROUPS = [[2 * z + k for z in range(8)] for k in range(2)]


def column_choice():
    table = np.zeros((96, 128), np.float32)
    for h in range(2):
        for m in range(32):
            al, k, q = m // 8, (m % 8) // 4, m % 4
            table[h * 48 + m, k * 32 + h * 16 + 4 * q + al] = 1
        for m in range(16):
            al, q = m // 4, m % 4
            table[h * 48 + 32 + m, 64 + h * 16 + 4 * q + al] = 1
    return table


def lane_order():
    table = np.zeros((512, 512), np.float32)
    for g in range(2):
        for al in range(4):
            for i in range(9):
                for q in range(4):
                    table[g * 256 + al * LINES + i * 4 + q, i * 32 + g * 16 + 4 * q + al] = 1
            for k in range(2):
                for q in range(4):
                    table[g * 256 + TALL + al * 8 + k * 4 + q, 384 + k * 32 + g * 16 + 4 * q + al] = 1
    return table


def dot(left, right):
    return jnp.dot(left, right, preferred_element_type=F32)


def halves(x):
    high = x.astype(BF16)
    return high, (x - high.astype(F32)).astype(BF16)


def thirds(x):
    high = x.astype(BF16)
    rest = x - high.astype(F32)
    mid = rest.astype(BF16)
    return high, mid, (rest - mid.astype(F32)).astype(BF16)


def product_terms(left, right):
    return dot(jnp.concatenate(halves(left), 0), jnp.concatenate(halves(right), 1))


def folded(terms):
    m, n = terms.shape[0] // 2, terms.shape[1] // 2
    return terms[:m, :n] + (terms[:m, n:] + terms[m:, :n])


def chosen(x, table):
    m = x.shape[0]
    out = dot(jnp.concatenate(thirds(x), 0), table)
    return out[:m] + (out[m : 2 * m] + out[2 * m :])


def lanes_of(shape):
    return lax.broadcasted_iota(jnp.int32, shape, len(shape) - 1)


def rank_body(where, s1, s2, tiles, packed, slot1, slot2, table, lhs, rhs, stage):
    col = where[1]
    upper = (
        lax.broadcasted_iota(jnp.int32, (128, 128), 0) < lax.broadcasted_iota(jnp.int32, (128, 128), 1)
    ).astype(BF16)
    groups = lax.broadcasted_iota(jnp.int32, (16, 128), 0)
    ranks = []
    for which, (source, target) in enumerate(((s1, slot1), (s2, slot2))):
        carry = jnp.zeros((16, 1), F32)
        rank = []
        for m in range(12):
            row = source[m : m + 1, :]
            group = jnp.bitwise_and(lax.shift_right_logical(row, 5), 15)
            inside = row < 4608
            mark = ((group == groups) & inside).astype(F32)
            before = dot(mark.astype(BF16), upper) + carry
            t = jnp.sum(mark * before, axis=0, keepdims=True)
            carry = carry + jnp.sum(mark, axis=1, keepdims=True)
            rank.append(t + 1.0)
            place = group * (2 * SLOTS) + which * SLOTS + t.astype(jnp.int32)
            if which:
                high = lax.shift_right_logical(row - 4608, 9)
                other = EXT + group * 64 + high * 32 + jnp.bitwise_and(row, 31)
                place = jnp.where(inside, place, other)
            target[m : m + 1, :] = place
        ranks.append(rank)
    slots = lanes_of((32, 128)).astype(F32)
    table[288:, :] = jnp.zeros((96, 256), BF16)
    for j in range(9):
        spots = lax.broadcasted_iota(jnp.int32, (32, 128), 0) + (j * 512 + col * 32)
        both = []
        for source, rank in ((s1, ranks[0]), (s2, ranks[1])):
            total = jnp.zeros((32, 128), F32)
            for m in range(12):
                total = total + jnp.where(source[m : m + 1, :] == spots, rank[m], 0.0)
            slot = jnp.sum(total, axis=1, keepdims=True) - 1.0
            both.append((slot == slots).astype(BF16))
        pair = jnp.concatenate(both, 1)
        table[j * 32 : (j + 1) * 32, :] = pair
        for al in range(4):
            rhs[j * 128 + al * 32 : j * 128 + (al + 1) * 32, :] = pair
        stage[...] = jnp.zeros((LINES, 128), F32)
        for i in range(9):
            stage[i * 4 : (i + 1) * 4, :] = tiles[i, j]
        x = stage[...]
        quarter = lanes_of((LINES, 128)) // 32
        x = jnp.concatenate([jnp.where(quarter == al, x, 0.0) for al in range(4)], 0)
        for part, value in enumerate(thirds(x)):
            lhs[part * TALL : (part + 1) * TALL, j * 128 : (j + 1) * 128] = value
    out = dot(lhs[...], rhs[...])
    packed[...] = out[:TALL] + (out[TALL : 2 * TALL] + out[2 * TALL :])


def second_body(slot2, panels, mixed, spread, fold, extra):
    spread[...] = jnp.zeros(spread.shape, F32)

    def place(step, _):
        x, y = step // 8, step % 8
        base = (y * 4 + x) * 48
        for u in range(48):
            spread[pl.ds(slot2[base + u], 1), :] = panels[x, y, u : u + 1, :]
        return 0

    lax.fori_loop(0, 32, place, 0)
    lane = lanes_of((40, 128))
    lane_r = lanes_of((64, 128))
    total = jnp.zeros((160, 256), F32)
    for c in range(16):
        x = mixed[c]
        left = jnp.concatenate([jnp.where(lane < 64, x, 0.0), jnp.where(lane >= 64, x, 0.0)], 0)
        right = spread[EXT + c * 64 : EXT + (c + 1) * 64, :]
        right = jnp.where((lane_r >= 64) & (lane_r < 96), right, 0.0)
        total = total + product_terms(left, jnp.concatenate([right, right], 0))
    out = folded(total)
    lane_f = lanes_of((16, 128))
    value = jnp.zeros((16, 128), F32)
    for h in range(3):
        moved = pltpu.roll(out[16 * h : 16 * (h + 1), :], (32 * h - 64) % 128, 1)
        value = jnp.where(lane_f // 32 == h, moved, value)
    fold[...] = value
    extra[...] = out[48:80, :]


def image_body(where, slot1, panels, fold, spread, blocks, extra, choice, right, send, comb):
    lane = lanes_of((16, 128))

    def join(step, _):
        x, y = step // 8, step % 8
        base = pl.multiple_of((y * 4 + x) * 48, 16)
        q = -fold[x, y]
        for h in range(3):
            moved = pltpu.roll(q, (64 - 32 * h) % 128, 1)
            value = jnp.where(lane < 64, panels[x, y, 16 * h : 16 * (h + 1), :], jnp.where(lane < 96, moved, 0.0))
            comb[pl.ds(base + 16 * h, 16), :] = value
        return 0

    lax.fori_loop(0, 32, join, 0)
    lane_r = lanes_of((SLOTS, 128))
    for c in range(16):
        low = c * 2 * SLOTS
        right[low : low + SLOTS, :] = jnp.zeros((SLOTS, 128), F32)
        value = spread[low + SLOTS : low + 2 * SLOTS, :]
        right[low + SLOTS : low + 2 * SLOTS, :] = jnp.where((lane_r >= 64) & (lane_r < 96), value, 0.0)

    def place(step, _):
        base = pl.multiple_of(step * 48, 16)
        for u in range(48):
            right[pl.ds(slot1[base + u], 1), :] = comb[pl.ds(base + u, 1), :]
        return 0

    lax.fori_loop(0, 32, place, 0)
    total = jnp.zeros((2 * TALL, 256), F32)
    for c in range(16):
        total = total + product_terms(blocks[c], right[c * 256 : (c + 1) * 256, :])
    image = jnp.concatenate([folded(total), extra[...]], 0)
    sent = jnp.zeros((96, TALL + 32), F32)
    for part in thirds(image):
        sent = sent + lax.dot_general(choice[...], part, (((1,), (1,)), ((), ())), preferred_element_type=F32)
    sent = jnp.concatenate([sent, jnp.zeros((96, 256 - TALL - 32), F32)], 1)
    parity = where[0] % 2
    for h in range(2):
        send[pl.ds((h + parity) % 2, 1)] = sent[h * 48 : (h + 1) * 48][None]


def cross_body(where, got0, got1, order, table, first, second, share, own):
    parity = where[0] % 2
    a, b = got0[...], got1[...]
    even = jnp.where(parity == 0, a, b)
    odd = jnp.where(parity == 0, b, a)
    y = chosen(jnp.concatenate([even, odd], 1), order[...])
    close = chosen(y[:, :384], table[...])
    share[0:48, :] = close[:, :128]
    share[48:64, :] = close[32:48, 128:]
    e = y[32:48, 384:512]
    own[...] = e
    lane = lanes_of((8, 128))
    share[64:72, :] = jnp.where(lane < 64, e[:8], pltpu.roll(e[8:], 64, 1))
    lane2 = lanes_of((4, 128))
    for i in range(9):
        chunk = (i // 4) * 128
        one = jnp.zeros((8, 128), F32)
        two = jnp.zeros((4, 128), F32)
        for al in range(4):
            shift = ((al - i % 4) * 32) % 128
            moved = pltpu.roll(y[al * 8 : (al + 1) * 8, chunk : chunk + 128], shift, 1) if shift else y[al * 8 : (al + 1) * 8, chunk : chunk + 128]
            one = jnp.where(lane // 32 == al, moved, one)
            low = y[32 + al * 4 : 36 + al * 4, chunk : chunk + 128]
            moved = pltpu.roll(low, shift, 1) if shift else low
            two = jnp.where(lane2 // 32 == al, moved, two)
        first[0, i] = -one[0:4]
        first[1, i] = -one[4:8]
        second[0, i] = -two


def diagonal_body(shares, right, spread, own, d1, d2, first, second):
    lane_r = lanes_of((64, 128))
    lane_e = lanes_of((8, 128))
    total = jnp.zeros((128, 256), F32)
    also = jnp.zeros((32, 256), F32)
    for c in range(16):
        x = shares[c]
        zero = jnp.zeros((48, 128), F32)
        left = jnp.concatenate(
            [jnp.concatenate([x[:48], zero], 1), jnp.concatenate([zero[:16], x[48:64]], 1)], 0
        )
        total = total + product_terms(left, right[c * 256 : (c + 1) * 256, :])
        e = x[64:72]
        left = jnp.concatenate([jnp.where(lane_e < 64, e, 0.0), jnp.where(lane_e >= 64, e, 0.0)], 0)
        v = spread[EXT + c * 64 : EXT + (c + 1) * 64, :]
        v = jnp.where((lane_r >= 64) & (lane_r < 96), v, 0.0)
        also = also + product_terms(left, jnp.concatenate([v, v], 0))
    out = folded(total)
    g1 = out[:32]
    bottom = own[...] - out[32:48]
    g2 = out[32:48] + out[48:64] + folded(also)
    lane = lanes_of((8, 128))
    lane2 = lanes_of((4, 128))
    for k in range(2):
        one = jnp.zeros((8, 128), F32)
        two = jnp.zeros((4, 128), F32)
        for al in range(4):
            shift = ((al - k) * 32) % 128
            one = jnp.where(lane // 32 == al, pltpu.roll(g1[al * 8 : (al + 1) * 8], shift, 1), one)
            two = jnp.where(lane2 // 32 == al, pltpu.roll(bottom[al * 4 : (al + 1) * 4], shift, 1), two)
        first[0, k] = d1[0, k] + one[0:4]
        first[1, k] = d1[1, k] + one[4:8]
        second[0, k] = -two
    two = jnp.zeros((4, 128), F32)
    for al in range(4):
        shift = ((al - 2) * 32) % 128
        two = jnp.where(lane2 // 32 == al, pltpu.roll(g2[al * 4 : (al + 1) * 4], shift, 1), two)
    second[0, 2] = d2[0, 0] + two


VMEM = pl.BlockSpec(memory_space=pltpu.VMEM)
SMEM = pl.BlockSpec(memory_space=pltpu.SMEM)


def kernel(body, specs, outs, scratch=()):
    return pl.pallas_call(
        body,
        in_specs=list(specs),
        out_specs=[VMEM] * len(outs),
        out_shape=[jax.ShapeDtypeStruct(shape, dtype) for shape, dtype in outs],
        scratch_shapes=list(scratch),
    )


def from_all(x, axis, count, groups=None):
    copies = jnp.broadcast_to(x, (count, *x.shape))
    return lax.all_to_all(copies, axis, 0, 0, axis_index_groups=groups, tiled=True)


def along_rows(x):
    return from_all(from_all(x, "row", 8, Y_GROUPS), "row", 4, X_GROUPS)


def along_cols(x):
    return from_all(x, "col", 16)


def transposed(x, turn):
    pairs = [(r * 16 + c, (2 * c + (r + turn) % 2) * 16 + r // 2) for r in range(32) for c in range(16)]
    return lax.ppermute(x, ("row", "col"), pairs)


def on_device(ancestor, inverse_first, panel_first, structure_first, inverse_second, panel_second, structure_second):
    where = jnp.stack([lax.axis_index("row"), lax.axis_index("col")]).astype(jnp.int32)
    p1 = panel_first.reshape(48, 64)
    p2 = panel_second.reshape(48, 32)
    panel = jnp.concatenate([p1, p2, jnp.zeros((48, 32), F32)], 1)
    d1 = inverse_first.reshape(2, 2, 4, 4, 32).transpose(3, 0, 2, 1, 4).reshape(32, 64)
    stacked = jnp.concatenate([p1, d1], 0)
    mixed = jnp.concatenate([stacked[:40], stacked[40:]], 1)

    packed, slot1, slot2, table = kernel(
        rank_body,
        (SMEM, VMEM, VMEM, VMEM),
        (((TALL, 256), F32), ((12, 128), jnp.int32), ((12, 128), jnp.int32), ((384, 256), BF16)),
        (pltpu.VMEM((3 * TALL, 1152), BF16), pltpu.VMEM((1152, 256), BF16), pltpu.VMEM((LINES, 128), F32)),
    )(where, structure_first.reshape(12, 128), structure_second.reshape(12, 128), ancestor)
    blocks = lax.all_gather(packed, "col")
    panels = along_rows(panel)
    mixes = along_cols(mixed)
    slot1, slot2 = slot1.reshape(1536), slot2.reshape(1536)
    spread, fold, extra = kernel(
        second_body,
        (SMEM, VMEM, VMEM),
        (((EXT + 1024, 128), F32), ((16, 128), F32), ((32, 128), F32)),
    )(slot2, panels, mixes)
    folds = along_rows(fold)
    right, send = kernel(
        image_body,
        (SMEM, SMEM, VMEM, VMEM, VMEM, VMEM, VMEM, VMEM),
        (((EXT, 128), F32), ((2, 48, 256), F32)),
        (pltpu.VMEM((1536, 128), F32),),
    )(where, slot1, panels, folds, spread, blocks, extra, jnp.asarray(column_choice(), BF16))
    got0, got1 = transposed(send[0], 0), transposed(send[1], 1)
    first_left, second_left, share, own = kernel(
        cross_body,
        (SMEM, VMEM, VMEM, VMEM, VMEM),
        (((2, 9, 4, 128), F32), ((1, 9, 4, 128), F32), ((72, 128), F32), ((16, 128), F32)),
    )(where, got0, got1, jnp.asarray(lane_order(), BF16), table)
    shares = along_cols(share)
    first_right, second_right = kernel(
        diagonal_body,
        (VMEM,) * 6,
        (((2, 2, 4, 128), F32), ((1, 3, 4, 128), F32)),
    )(shares, right, spread, own, inverse_first, inverse_second)
    return (
        jnp.concatenate([first_left, first_right], 1),
        jnp.concatenate([second_left, second_right], 1),
    )


def solution(mesh):
    tiles = P(None, None, "row", "col")
    panels = P("row", None, "col")
    return jax.shard_map(
        on_device,
        mesh=mesh,
        in_specs=(tiles, tiles, panels, P(), tiles, panels, P()),
        out_specs=(tiles, tiles),
        check_vma=False,
    )
```

```python
import jax
import jax.numpy as jnp
import numpy as np
from jax import lax
from jax.experimental import pallas as pl
from jax.experimental.pallas import tpu as pltpu
from jax.sharding import PartitionSpec as P

F32 = jnp.float32
BF16 = jnp.bfloat16
LINES = 40
TALL = 4 * LINES
SLOTS = 128
EXT = 16 * SLOTS

Y_GROUPS = [[4 * y + x for y in range(8)] for x in range(4)]
X_GROUPS = [[4 * y + x for x in range(4)] for y in range(8)]
Z_GROUPS = [[2 * z + k for z in range(8)] for k in range(2)]


def column_choice():
    table = np.zeros((96, 128), np.float32)
    for h in range(2):
        for m in range(32):
            al, k, q = m // 8, (m % 8) // 4, m % 4
            table[h * 48 + m, k * 32 + h * 16 + 4 * q + al] = 1
        for m in range(16):
            al, q = m // 4, m % 4
            table[h * 48 + 32 + m, 64 + h * 16 + 4 * q + al] = 1
    return table


def lane_order():
    table = np.zeros((512, 512), np.float32)
    for g in range(2):
        for al in range(4):
            for i in range(9):
                for q in range(4):
                    table[g * 256 + al * LINES + i * 4 + q, i * 32 + g * 16 + 4 * q + al] = 1
            for k in range(2):
                for q in range(4):
                    table[g * 256 + TALL + al * 8 + k * 4 + q, 384 + k * 32 + g * 16 + 4 * q + al] = 1
    return table


def dot(left, right):
    return jnp.dot(left, right, preferred_element_type=F32)


def halves(x):
    high = x.astype(BF16)
    return high, (x - high.astype(F32)).astype(BF16)


def thirds(x):
    high = x.astype(BF16)
    rest = x - high.astype(F32)
    mid = rest.astype(BF16)
    return high, mid, (rest - mid.astype(F32)).astype(BF16)


def product_terms(left, right):
    return dot(jnp.concatenate(halves(left), 0), jnp.concatenate(halves(right), 1))


def folded(terms):
    m, n = terms.shape[0] // 2, terms.shape[1] // 2
    return terms[:m, :n] + (terms[:m, n:] + terms[m:, :n])


def chosen(x, table):
    m = x.shape[0]
    out = dot(jnp.concatenate(thirds(x), 0), table)
    return out[:m] + (out[m : 2 * m] + out[2 * m :])


def lanes_of(shape):
    return lax.broadcasted_iota(jnp.int32, shape, len(shape) - 1)


def rank_body(where, s1, s2, tiles, packed, slot1, slot2, table, lhs, rhs, stage):
    col = where[1]
    upper = (
        lax.broadcasted_iota(jnp.int32, (128, 128), 0) < lax.broadcasted_iota(jnp.int32, (128, 128), 1)
    ).astype(BF16)
    groups = lax.broadcasted_iota(jnp.int32, (16, 128), 0)
    ranks = []
    for which, (source, target) in enumerate(((s1, slot1), (s2, slot2))):
        carry = jnp.zeros((16, 1), F32)
        rank = []
        for m in range(12):
            row = source[m : m + 1, :]
            group = jnp.bitwise_and(lax.shift_right_logical(row, 5), 15)
            inside = row < 4608
            mark = ((group == groups) & inside).astype(F32)
            before = dot(mark.astype(BF16), upper) + carry
            t = jnp.sum(mark * before, axis=0, keepdims=True)
            carry = carry + jnp.sum(mark, axis=1, keepdims=True)
            rank.append(t + 1.0)
            place = group * SLOTS + t.astype(jnp.int32)
            if which:
                high = lax.shift_right_logical(row - 4608, 9)
                other = EXT + group * 64 + high * 32 + jnp.bitwise_and(row, 31)
                place = jnp.where(inside, place, other)
            target[m : m + 1, :] = place
        ranks.append(rank)
    slots = lanes_of((32, 128)).astype(F32)
    table[288:, :] = jnp.zeros((96, 256), BF16)
    for j in range(9):
        spots = lax.broadcasted_iota(jnp.int32, (32, 128), 0) + (j * 512 + col * 32)
        both = []
        for source, rank in ((s1, ranks[0]), (s2, ranks[1])):
            total = jnp.zeros((32, 128), F32)
            for m in range(12):
                total = total + jnp.where(source[m : m + 1, :] == spots, rank[m], 0.0)
            slot = jnp.sum(total, axis=1, keepdims=True) - 1.0
            both.append((slot == slots).astype(BF16))
        pair = jnp.concatenate(both, 1)
        table[j * 32 : (j + 1) * 32, :] = pair
        for al in range(4):
            rhs[j * 128 + al * 32 : j * 128 + (al + 1) * 32, :] = pair
        stage[...] = jnp.zeros((LINES, 128), F32)
        for i in range(9):
            stage[i * 4 : (i + 1) * 4, :] = tiles[i, j]
        x = stage[...]
        quarter = lanes_of((LINES, 128)) // 32
        x = jnp.concatenate([jnp.where(quarter == al, x, 0.0) for al in range(4)], 0)
        for part, value in enumerate(thirds(x)):
            lhs[part * TALL : (part + 1) * TALL, j * 128 : (j + 1) * 128] = value
    out = dot(lhs[...], rhs[...])
    packed[...] = out[:TALL] + (out[TALL : 2 * TALL] + out[2 * TALL :])


def lay_body(p1, p2, d1, panel, mixed, tall):
    tall[...] = jnp.zeros((128, 128), F32)
    tall[0:32, 0:48] = p1[0]
    tall[32:64, 0:48] = p1[1]
    tall[64:96, 0:48] = p2[0]
    both = tall[...].T[:48]
    for n in range(8):
        panel[n] = both
    lane = lanes_of((4, 128))
    tall[0:48, :] = both
    for al in range(4):
        for k in range(2):
            value = jnp.zeros((4, 128), F32)
            for m in range(2):
                value = jnp.where(lane // 32 == m, pltpu.roll(d1[k, m], ((m - al) * 32) % 128, 1), value)
            tall[48 + al * 8 + k * 4 : 52 + al * 8 + k * 4, :] = value
    half = lanes_of((40, 128)) < 64
    value = jnp.where(half, tall[0:40, :], pltpu.roll(tall[40:80, :], 64, 1))
    for n in range(8):
        mixed[n] = value


def scatter_rows(slots, source, target):
    def place(step, _):
        base = pl.multiple_of(step * 48, 16)
        for u in range(48):
            target[pl.ds(slots[base + u], 1), :] = source[pl.ds(base + u, 1), :]
        return 0

    lax.fori_loop(0, 32, place, 0)


def in_order(step):
    return pl.multiple_of(((step % 8) * 4 + step // 8) * 48, 16)


def second_body(where, slot2, panels, mine, other, spread, fold, extra, rows):
    lane = lanes_of((48, 128))
    keep = (lane >= 64) & (lane < 96)

    def copy(step, _):
        rows[pl.ds(in_order(step), 48), :] = jnp.where(keep, panels[step // 8, step % 8], 0.0)
        return 0

    lax.fori_loop(0, 32, copy, 0)
    spread[...] = jnp.zeros(spread.shape, F32)
    scatter_rows(slot2, rows, spread)
    core = where[1] % 2
    half = lanes_of((40, 128)) < 64
    total = jnp.zeros((160, 256), F32)
    for z in range(8):
        for source, k in ((mine, core), (other, 1 - core)):
            x = source[z]
            left = jnp.concatenate([jnp.where(half, x, 0.0), jnp.where(half, 0.0, x)], 0)
            right = spread[pl.ds(pl.multiple_of(EXT + (2 * z + k) * 64, 64), 64), :]
            total = total + product_terms(left, jnp.concatenate([right, right], 0))
    out = folded(total)
    lane_f = lanes_of((16, 128))
    value = jnp.zeros((16, 128), F32)
    for h in range(3):
        moved = pltpu.roll(out[16 * h : 16 * (h + 1), :], (32 * h - 64) % 128, 1)
        value = jnp.where(lane_f // 32 == h, moved, value)
    for n in range(8):
        fold[n] = value
    extra[...] = out[48:80, :]


def first_body(slot1, panels, spread, rows):
    keep = lanes_of((48, 128)) < 64

    def copy(step, _):
        rows[pl.ds(in_order(step), 48), :] = jnp.where(keep, panels[step // 8, step % 8], 0.0)
        return 0

    lax.fori_loop(0, 32, copy, 0)
    spread[...] = jnp.zeros(spread.shape, F32)
    scatter_rows(slot1, rows, spread)


def image_body(where, slot1, fold, own, second, blocks, extra, choice, right, send0, send1, rows, held, done):
    send = (send0, send1)
    arrival = pltpu.make_async_copy(blocks, held, done)
    arrival.start()
    keep = lanes_of((16, 128))
    keep = (keep >= 64) & (keep < 96)

    def join(step, _):
        q = -fold[step // 8, step % 8]
        base = in_order(step)
        for h in range(3):
            moved = pltpu.roll(q, (64 - 32 * h) % 128, 1)
            rows[pl.ds(base + 16 * h, 16), :] = jnp.where(keep, moved, 0.0)
        return 0

    lax.fori_loop(0, 32, join, 0)
    right[...] = jnp.zeros(right.shape, F32)
    scatter_rows(slot1, rows, right)
    right[...] = right[...] + own[...]
    arrival.wait()
    total = jnp.zeros((2 * TALL, 256), F32)
    for c in range(16):
        part = slice(c * SLOTS, (c + 1) * SLOTS)
        total = total + product_terms(held[c], jnp.concatenate([right[part, :], second[part, :]], 0))
    image = jnp.concatenate([folded(total), extra[...]], 0)
    sent = jnp.zeros((96, TALL + 32), F32)
    for part in thirds(image):
        sent = sent + lax.dot_general(choice[...], part, (((1,), (1,)), ((), ())), preferred_element_type=F32)
    sent = jnp.concatenate([sent, jnp.zeros((96, 256 - TALL - 32), F32)], 1)
    parity = where[0] % 2
    for h in range(2):

        @pl.when(parity == h)
        def _(h=h):
            send[0][...] = sent[h * 48 : (h + 1) * 48]
            send[1][...] = sent[(1 - h) * 48 : (2 - h) * 48]


def cross_body(where, got0, got1, order, table, first, second, share, own):
    parity = where[0] % 2
    a, b = got0[...], got1[...]
    even = jnp.where(parity == 0, a, b)
    odd = jnp.where(parity == 0, b, a)
    y = chosen(jnp.concatenate([even, odd], 1), order[...])
    close = chosen(y[:, :384], table[...])
    e = y[32:48, 384:512]
    own[...] = e
    lane = lanes_of((8, 128))
    e = jnp.where(lane < 64, e[:8], pltpu.roll(e[8:], 64, 1))
    e = jnp.concatenate([close[:, :128], close[32:48, 128:], e], 0)
    for n in range(8):
        share[n] = e
    lane2 = lanes_of((4, 128))
    for i in range(9):
        chunk = (i // 4) * 128
        one = jnp.zeros((8, 128), F32)
        two = jnp.zeros((4, 128), F32)
        for al in range(4):
            shift = ((al - i % 4) * 32) % 128
            moved = pltpu.roll(y[al * 8 : (al + 1) * 8, chunk : chunk + 128], shift, 1) if shift else y[al * 8 : (al + 1) * 8, chunk : chunk + 128]
            one = jnp.where(lane // 32 == al, moved, one)
            low = y[32 + al * 4 : 36 + al * 4, chunk : chunk + 128]
            moved = pltpu.roll(low, shift, 1) if shift else low
            two = jnp.where(lane2 // 32 == al, moved, two)
        first[0, i] = -one[0:4]
        first[1, i] = -one[4:8]
        second[0, i] = -two


def diagonal_body(where, mine, other, right, spread, own, d1, d2, left1, left2, first, second):
    first[:, 0:9] = left1[...]
    second[:, 0:9] = left2[...]
    core = where[1] % 2
    lane_e = lanes_of((8, 128))
    total = jnp.zeros((128, 256), F32)
    also = jnp.zeros((32, 256), F32)
    for z in range(8):
        for source, k in ((mine, core), (other, 1 - core)):
            c = 2 * z + k
            x = source[z]
            part = pl.ds(pl.multiple_of(c * SLOTS, SLOTS), SLOTS)
            zero = jnp.zeros((48, 128), F32)
            left = jnp.concatenate(
                [jnp.concatenate([x[:48], zero], 1), jnp.concatenate([zero[:16], x[48:64]], 1)], 0
            )
            total = total + product_terms(left, jnp.concatenate([right[part, :], spread[part, :]], 0))
            e = x[64:72]
            left = jnp.concatenate([jnp.where(lane_e < 64, e, 0.0), jnp.where(lane_e >= 64, e, 0.0)], 0)
            v = spread[pl.ds(pl.multiple_of(EXT + c * 64, 64), 64), :]
            also = also + product_terms(left, jnp.concatenate([v, v], 0))
    out = folded(total)
    g1 = out[:32]
    bottom = own[...] - out[32:48]
    g2 = out[32:48] + out[48:64] + folded(also)
    lane = lanes_of((8, 128))
    lane2 = lanes_of((4, 128))
    for k in range(2):
        one = jnp.zeros((8, 128), F32)
        two = jnp.zeros((4, 128), F32)
        for al in range(4):
            shift = ((al - k) * 32) % 128
            one = jnp.where(lane // 32 == al, pltpu.roll(g1[al * 8 : (al + 1) * 8], shift, 1), one)
            two = jnp.where(lane2 // 32 == al, pltpu.roll(bottom[al * 4 : (al + 1) * 4], shift, 1), two)
        first[0, 9 + k] = d1[0, k] + one[0:4]
        first[1, 9 + k] = d1[1, k] + one[4:8]
        second[0, 9 + k] = -two
    two = jnp.zeros((4, 128), F32)
    for al in range(4):
        shift = ((al - 2) * 32) % 128
        two = jnp.where(lane2 // 32 == al, pltpu.roll(g2[al * 4 : (al + 1) * 4], shift, 1), two)
    second[0, 11] = d2[0, 0] + two


VMEM = pl.BlockSpec(memory_space=pltpu.VMEM)
SMEM = pl.BlockSpec(memory_space=pltpu.SMEM)
ANY = pl.BlockSpec(memory_space=pl.ANY)


def kernel(body, specs, outs, scratch=()):
    return pl.pallas_call(
        body,
        in_specs=list(specs),
        out_specs=[VMEM] * len(outs),
        out_shape=[jax.ShapeDtypeStruct(shape, dtype) for shape, dtype in outs],
        scratch_shapes=list(scratch),
    )


def exchanged(x, axis, groups):
    return lax.all_to_all(x, axis, 0, 0, axis_index_groups=groups, tiled=True)


def along_rows(x):
    near = exchanged(x, "row", Y_GROUPS)
    return exchanged(jnp.broadcast_to(near, (4, *near.shape)), "row", X_GROUPS)


def along_cols(x):
    mine = exchanged(x, "col", Z_GROUPS)
    return mine, lax.ppermute(mine, "col", [(c, c ^ 1) for c in range(16)])


def transposed(x, turn):
    pairs = [(r * 16 + c, (2 * c + (r + turn) % 2) * 16 + r // 2) for r in range(32) for c in range(16)]
    return lax.ppermute(x, ("row", "col"), pairs)


def on_device(ancestor, inverse_first, panel_first, structure_first, inverse_second, panel_second, structure_second):
    where = jnp.stack([lax.axis_index("row"), lax.axis_index("col")]).astype(jnp.int32)
    panel, mixed = kernel(
        lay_body,
        (VMEM, VMEM, VMEM),
        (((8, 48, 128), F32), ((8, 40, 128), F32)),
        (pltpu.VMEM((128, 128), F32),),
    )(panel_first.transpose(1, 2, 0), panel_second.transpose(1, 2, 0), inverse_first)
    packed, slot1, slot2, table = kernel(
        rank_body,
        (SMEM, VMEM, VMEM, VMEM),
        (((TALL, 256), F32), ((12, 128), jnp.int32), ((12, 128), jnp.int32), ((384, 256), BF16)),
        (pltpu.VMEM((3 * TALL, 1152), BF16), pltpu.VMEM((1152, 256), BF16), pltpu.VMEM((LINES, 128), F32)),
    )(where, structure_first.reshape(12, 128), structure_second.reshape(12, 128), ancestor)
    blocks = lax.all_gather(packed, "col")
    panels = along_rows(panel)
    mine, other = along_cols(mixed)
    slot1, slot2 = slot1.reshape(1536), slot2.reshape(1536)
    rows = pltpu.VMEM((1536, 128), F32)
    spread, fold, extra = kernel(
        second_body,
        (SMEM, SMEM, VMEM, VMEM, VMEM),
        (((EXT + 1024, 128), F32), ((8, 16, 128), F32), ((32, 128), F32)),
        (rows,),
    )(where, slot2, panels, mine, other)
    folds = along_rows(fold)
    (own,) = kernel(first_body, (SMEM, VMEM), (((EXT, 128), F32),), (rows,))(slot1, panels)
    right, send0, send1 = kernel(
        image_body,
        (SMEM, SMEM, VMEM, VMEM, VMEM, ANY, VMEM, VMEM),
        (((EXT, 128), F32), ((48, 256), F32), ((48, 256), F32)),
        (rows, pltpu.VMEM((16, TALL, 256), F32), pltpu.SemaphoreType.DMA),
    )(where, slot1, folds, own, spread, blocks, extra, jnp.asarray(column_choice(), BF16))
    got0, got1 = transposed(send0, 0), transposed(send1, 1)
    left1, left2, share, own = kernel(
        cross_body,
        (SMEM, VMEM, VMEM, VMEM, VMEM),
        (((2, 9, 4, 128), F32), ((1, 9, 4, 128), F32), ((8, 72, 128), F32), ((16, 128), F32)),
    )(where, got0, got1, jnp.asarray(lane_order(), BF16), table)
    mine, other = along_cols(share)
    return kernel(
        diagonal_body,
        (SMEM,) + (VMEM,) * 9,
        (((2, 11, 4, 128), F32), ((1, 12, 4, 128), F32)),
    )(where, mine, other, right, spread, own, inverse_first, inverse_second, left1, left2)


def solution(mesh):
    tiles = P(None, None, "row", "col")
    panels = P("row", None, "col")
    return jax.shard_map(
        on_device,
        mesh=mesh,
        in_specs=(tiles, tiles, panels, P(), tiles, panels, P()),
        out_specs=(tiles, tiles),
        check_vma=False,
    )
```

```python
import jax
import jax.numpy as jnp
import numpy as np
from jax import lax
from jax.experimental import pallas as pl
from jax.experimental.pallas import tpu as pltpu
from jax.sharding import PartitionSpec as P

F32 = jnp.float32
BF16 = jnp.bfloat16
TALL = 144
SLOTS = 128
EXT = 16 * SLOTS

Y_GROUPS = [[4 * y + x for y in range(8)] for x in range(4)]
X_GROUPS = [[4 * y + x for x in range(4)] for y in range(8)]
Z_GROUPS = [[2 * z + k for z in range(8)] for k in range(2)]


def column_choice():
    table = np.zeros((96, 128), np.float32)
    for h in range(2):
        for m in range(32):
            al, k, q = m // 8, (m % 8) // 4, m % 4
            table[h * 48 + m, k * 32 + h * 16 + 4 * q + al] = 1
        for m in range(16):
            al, q = m // 4, m % 4
            table[h * 48 + 32 + m, 64 + h * 16 + 4 * q + al] = 1
    return table


def lane_order():
    table = np.zeros((512, 512), np.float32)
    for g in range(2):
        for al in range(4):
            for i in range(9):
                for q in range(4):
                    table[g * 256 + i * 16 + al * 4 + q, i * 32 + g * 16 + 4 * q + al] = 1
            for k in range(2):
                for q in range(4):
                    table[g * 256 + TALL + al * 8 + k * 4 + q, 384 + k * 32 + g * 16 + 4 * q + al] = 1
    return table


def dot(left, right):
    return jnp.dot(left, right, preferred_element_type=F32)


def halves(x):
    high = x.astype(BF16)
    return high, (x - high.astype(F32)).astype(BF16)


def thirds(x):
    high = x.astype(BF16)
    rest = x - high.astype(F32)
    mid = rest.astype(BF16)
    return high, mid, (rest - mid.astype(F32)).astype(BF16)


def product_terms(left, right):
    return dot(jnp.concatenate(halves(left), 0), jnp.concatenate(halves(right), 1))


def folded(terms):
    m, n = terms.shape[0] // 2, terms.shape[1] // 2
    return terms[:m, :n] + (terms[:m, n:] + terms[m:, :n])


def chosen(x, table):
    m = x.shape[0]
    out = dot(jnp.concatenate(thirds(x), 0), table)
    return out[:m] + (out[m : 2 * m] + out[2 * m :])


def lanes_of(shape):
    return lax.broadcasted_iota(jnp.int32, shape, len(shape) - 1)


def rank_body(where, s1, s2, tiles, packed, slot1, slot2, table, lhs, rhs, stage):
    col = where[1]
    upper = (
        lax.broadcasted_iota(jnp.int32, (128, 128), 0) < lax.broadcasted_iota(jnp.int32, (128, 128), 1)
    ).astype(BF16)
    groups = lax.broadcasted_iota(jnp.int32, (16, 128), 0)
    ranks = []
    for which, (source, target) in enumerate(((s1, slot1), (s2, slot2))):
        carry = jnp.zeros((16, 1), F32)
        rank = []
        for m in range(12):
            row = source[m : m + 1, :]
            group = jnp.bitwise_and(lax.shift_right_logical(row, 5), 15)
            inside = row < 4608
            mark = ((group == groups) & inside).astype(F32)
            before = dot(mark.astype(BF16), upper) + carry
            t = jnp.sum(mark * before, axis=0, keepdims=True)
            carry = carry + jnp.sum(mark, axis=1, keepdims=True)
            rank.append(t + 1.0)
            place = group * SLOTS + t.astype(jnp.int32)
            if which:
                high = lax.shift_right_logical(row - 4608, 9)
                other = EXT + group * 64 + high * 32 + jnp.bitwise_and(row, 31)
                place = jnp.where(inside, place, other)
            target[m : m + 1, :] = place
        ranks.append(rank)
    slots = lanes_of((32, 128)).astype(F32)
    table[288:, :] = jnp.zeros((96, 256), BF16)
    for j in range(9):
        spots = lax.broadcasted_iota(jnp.int32, (32, 128), 0) + (j * 512 + col * 32)
        both = []
        for source, rank in ((s1, ranks[0]), (s2, ranks[1])):
            total = jnp.zeros((32, 128), F32)
            for m in range(12):
                total = total + jnp.where(source[m : m + 1, :] == spots, rank[m], 0.0)
            slot = jnp.sum(total, axis=1, keepdims=True) - 1.0
            both.append((slot == slots).astype(BF16))
        pair = jnp.concatenate(both, 1)
        table[j * 32 : (j + 1) * 32, :] = pair
        for al in range(4):
            rhs[j * 128 + al * 32 : j * 128 + (al + 1) * 32, :] = pair
        quarter = lanes_of((4, 128)) // 32
        for i in range(9):
            for al in range(4):
                stage[i * 16 + al * 4 : i * 16 + (al + 1) * 4, :] = jnp.where(quarter == al, tiles[i, j], 0.0)
        for part, value in enumerate(thirds(stage[...])):
            lhs[part * TALL : (part + 1) * TALL, j * 128 : (j + 1) * 128] = value
    out = dot(lhs[...], rhs[...])
    packed[...] = out[:TALL] + (out[TALL : 2 * TALL] + out[2 * TALL :])


def lay_body(p1, p2, d1, panel, mixed, tall):
    tall[...] = jnp.zeros((128, 128), F32)
    tall[0:32, 0:48] = p1[0]
    tall[32:64, 0:48] = p1[1]
    tall[64:96, 0:48] = p2[0]
    both = tall[...].T[:48]
    for n in range(8):
        panel[n] = both
    lane = lanes_of((4, 128))
    tall[0:48, :] = both
    for al in range(4):
        for k in range(2):
            value = jnp.zeros((4, 128), F32)
            for m in range(2):
                value = jnp.where(lane // 32 == m, pltpu.roll(d1[k, m], ((m - al) * 32) % 128, 1), value)
            tall[48 + al * 8 + k * 4 : 52 + al * 8 + k * 4, :] = value
    half = lanes_of((40, 128)) < 64
    value = jnp.where(half, tall[0:40, :], pltpu.roll(tall[40:80, :], 64, 1))
    for n in range(8):
        mixed[n] = value


def scatter_rows(slots, source, target):
    def place(step, _):
        base = pl.multiple_of(step * 48, 16)
        for u in range(48):
            target[pl.ds(slots[base + u], 1), :] = source[pl.ds(base + u, 1), :]
        return 0

    lax.fori_loop(0, 32, place, 0)


def in_order(step):
    return pl.multiple_of(((step % 8) * 4 + step // 8) * 48, 16)


def second_body(where, slot2, panels, mine, other, spread, fold, extra, rows):
    lane = lanes_of((48, 128))
    keep = (lane >= 64) & (lane < 96)

    def copy(step, _):
        rows[pl.ds(in_order(step), 48), :] = jnp.where(keep, panels[step // 8, step % 8], 0.0)
        return 0

    lax.fori_loop(0, 32, copy, 0)
    spread[...] = jnp.zeros(spread.shape, F32)
    scatter_rows(slot2, rows, spread)
    core = where[1] % 2
    half = lanes_of((40, 128)) < 64
    total = jnp.zeros((160, 256), F32)
    for z in range(8):
        for source, k in ((mine, core), (other, 1 - core)):
            x = source[z]
            left = jnp.concatenate([jnp.where(half, x, 0.0), jnp.where(half, 0.0, x)], 0)
            right = spread[pl.ds(pl.multiple_of(EXT + (2 * z + k) * 64, 64), 64), :]
            total = total + product_terms(left, jnp.concatenate([right, right], 0))
    out = folded(total)
    lane_f = lanes_of((16, 128))
    value = jnp.zeros((16, 128), F32)
    for h in range(3):
        moved = pltpu.roll(out[16 * h : 16 * (h + 1), :], (32 * h - 64) % 128, 1)
        value = jnp.where(lane_f // 32 == h, moved, value)
    for n in range(32):
        fold[n] = value
    extra[...] = out[48:80, :]


def first_body(slot1, panels, spread, rows):
    keep = lanes_of((48, 128)) < 64

    def copy(step, _):
        rows[pl.ds(in_order(step), 48), :] = jnp.where(keep, panels[step // 8, step % 8], 0.0)
        return 0

    lax.fori_loop(0, 32, copy, 0)
    spread[...] = jnp.zeros(spread.shape, F32)
    scatter_rows(slot1, rows, spread)


def image_body(where, slot1, fold, own, second, blocks, extra, choice, right, send0, send1, rows, held, done):
    send = (send0, send1)
    arrival = pltpu.make_async_copy(blocks, held, done)
    arrival.start()
    keep = lanes_of((16, 128))
    keep = (keep >= 64) & (keep < 96)

    def join(step, _):
        q = -fold[step]
        base = pl.multiple_of(step * 48, 16)
        for h in range(3):
            moved = pltpu.roll(q, (64 - 32 * h) % 128, 1)
            rows[pl.ds(base + 16 * h, 16), :] = jnp.where(keep, moved, 0.0)
        return 0

    lax.fori_loop(0, 32, join, 0)
    right[...] = jnp.zeros(right.shape, F32)
    scatter_rows(slot1, rows, right)
    right[...] = right[...] + own[...]
    arrival.wait()
    total = jnp.zeros((2 * TALL, 256), F32)
    for c in range(16):
        part = slice(c * SLOTS, (c + 1) * SLOTS)
        total = total + product_terms(held[c], jnp.concatenate([right[part, :], second[part, :]], 0))
    image = jnp.concatenate([folded(total), extra[...]], 0)
    sent = jnp.zeros((96, TALL + 32), F32)
    for part in thirds(image):
        sent = sent + lax.dot_general(choice[...], part, (((1,), (1,)), ((), ())), preferred_element_type=F32)
    lane = lanes_of((16, 128))
    pieces = []
    for h in range(2):
        rest = jnp.concatenate([sent[h * 48 : (h + 1) * 48, 128:], jnp.zeros((48, 80), F32)], 1)
        tail = jnp.where(lane < 16, rest[0:16], pltpu.roll(rest[16:32], 16, 1))
        tail = jnp.where(lane < 32, tail, pltpu.roll(rest[32:48], 32, 1))
        pieces.append(jnp.concatenate([sent[h * 48 : (h + 1) * 48, :128], tail], 0))
    parity = where[0] % 2
    for h in range(2):

        @pl.when(parity == h)
        def _(h=h):
            send[0][...] = pieces[h]
            send[1][...] = pieces[1 - h]


def cross_body(where, got0, got1, order, table, first, second, share, own):
    parity = where[0] % 2
    a, b = got0[...], got1[...]
    even = jnp.where(parity == 0, a, b)
    odd = jnp.where(parity == 0, b, a)
    parts = []
    for got in (even, odd):
        tail = got[48:64]
        parts.append(got[:48])
        parts.append(jnp.concatenate([tail, pltpu.roll(tail, 112, 1), pltpu.roll(tail, 96, 1)], 0))
    y = chosen(jnp.concatenate(parts, 1), order[...])
    close = chosen(y[:, :384], table[...])
    e = y[32:48, 384:512]
    own[...] = e
    lane = lanes_of((8, 128))
    e = jnp.where(lane < 64, e[:8], pltpu.roll(e[8:], 64, 1))
    e = jnp.concatenate([close[:, :128], close[32:48, 128:], e], 0)
    for n in range(8):
        share[n] = e
    lane2 = lanes_of((4, 128))
    for i in range(9):
        chunk = (i // 4) * 128
        one = jnp.zeros((8, 128), F32)
        two = jnp.zeros((4, 128), F32)
        for al in range(4):
            shift = ((al - i % 4) * 32) % 128
            moved = pltpu.roll(y[al * 8 : (al + 1) * 8, chunk : chunk + 128], shift, 1) if shift else y[al * 8 : (al + 1) * 8, chunk : chunk + 128]
            one = jnp.where(lane // 32 == al, moved, one)
            low = y[32 + al * 4 : 36 + al * 4, chunk : chunk + 128]
            moved = pltpu.roll(low, shift, 1) if shift else low
            two = jnp.where(lane2 // 32 == al, moved, two)
        first[0, i] = -one[0:4]
        first[1, i] = -one[4:8]
        second[0, i] = -two


def diagonal_body(where, mine, other, right, spread, own, d1, d2, left1, left2, first, second):
    first[:, 0:9] = left1[...]
    second[:, 0:9] = left2[...]
    core = where[1] % 2
    lane_e = lanes_of((8, 128))
    total = jnp.zeros((128, 256), F32)
    also = jnp.zeros((32, 256), F32)
    for z in range(8):
        for source, k in ((mine, core), (other, 1 - core)):
            c = 2 * z + k
            x = source[z]
            part = pl.ds(pl.multiple_of(c * SLOTS, SLOTS), SLOTS)
            zero = jnp.zeros((48, 128), F32)
            left = jnp.concatenate(
                [jnp.concatenate([x[:48], zero], 1), jnp.concatenate([zero[:16], x[48:64]], 1)], 0
            )
            total = total + product_terms(left, jnp.concatenate([right[part, :], spread[part, :]], 0))
            e = x[64:72]
            left = jnp.concatenate([jnp.where(lane_e < 64, e, 0.0), jnp.where(lane_e >= 64, e, 0.0)], 0)
            v = spread[pl.ds(pl.multiple_of(EXT + c * 64, 64), 64), :]
            also = also + product_terms(left, jnp.concatenate([v, v], 0))
    out = folded(total)
    g1 = out[:32]
    bottom = own[...] - out[32:48]
    g2 = out[32:48] + out[48:64] + folded(also)
    lane = lanes_of((8, 128))
    lane2 = lanes_of((4, 128))
    for k in range(2):
        one = jnp.zeros((8, 128), F32)
        two = jnp.zeros((4, 128), F32)
        for al in range(4):
            shift = ((al - k) * 32) % 128
            one = jnp.where(lane // 32 == al, pltpu.roll(g1[al * 8 : (al + 1) * 8], shift, 1), one)
            two = jnp.where(lane2 // 32 == al, pltpu.roll(bottom[al * 4 : (al + 1) * 4], shift, 1), two)
        first[0, 9 + k] = d1[0, k] + one[0:4]
        first[1, 9 + k] = d1[1, k] + one[4:8]
        second[0, 9 + k] = -two
    two = jnp.zeros((4, 128), F32)
    for al in range(4):
        shift = ((al - 2) * 32) % 128
        two = jnp.where(lane2 // 32 == al, pltpu.roll(g2[al * 4 : (al + 1) * 4], shift, 1), two)
    second[0, 11] = d2[0, 0] + two


VMEM = pl.BlockSpec(memory_space=pltpu.VMEM)
SMEM = pl.BlockSpec(memory_space=pltpu.SMEM)
ANY = pl.BlockSpec(memory_space=pl.ANY)


def kernel(body, specs, outs, scratch=()):
    return pl.pallas_call(
        body,
        in_specs=list(specs),
        out_specs=[VMEM] * len(outs),
        out_shape=[jax.ShapeDtypeStruct(shape, dtype) for shape, dtype in outs],
        scratch_shapes=list(scratch),
    )


def exchanged(x, axis, groups):
    return lax.all_to_all(x, axis, 0, 0, axis_index_groups=groups, tiled=True)


def along_rows(x):
    near = exchanged(x, "row", Y_GROUPS)
    return exchanged(jnp.broadcast_to(near, (4, *near.shape)), "row", X_GROUPS)


def along_cols(x):
    mine = exchanged(x, "col", Z_GROUPS)
    return mine, lax.ppermute(mine, "col", [(c, c ^ 1) for c in range(16)])


def transposed(x, turn):
    pairs = [(r * 16 + c, (2 * c + (r + turn) % 2) * 16 + r // 2) for r in range(32) for c in range(16)]
    return lax.ppermute(x, ("row", "col"), pairs)


def on_device(ancestor, inverse_first, panel_first, structure_first, inverse_second, panel_second, structure_second):
    where = jnp.stack([lax.axis_index("row"), lax.axis_index("col")]).astype(jnp.int32)
    panel, mixed = kernel(
        lay_body,
        (VMEM, VMEM, VMEM),
        (((8, 48, 128), F32), ((8, 40, 128), F32)),
        (pltpu.VMEM((128, 128), F32),),
    )(panel_first.transpose(1, 2, 0), panel_second.transpose(1, 2, 0), inverse_first)
    packed, slot1, slot2, table = kernel(
        rank_body,
        (SMEM, VMEM, VMEM, VMEM),
        (((TALL, 256), F32), ((12, 128), jnp.int32), ((12, 128), jnp.int32), ((384, 256), BF16)),
        (pltpu.VMEM((3 * TALL, 1152), BF16), pltpu.VMEM((1152, 256), BF16), pltpu.VMEM((TALL, 128), F32)),
    )(where, structure_first.reshape(12, 128), structure_second.reshape(12, 128), ancestor)
    blocks = lax.all_gather(packed, "col")
    panels = along_rows(panel)
    mine, other = along_cols(mixed)
    slot1, slot2 = slot1.reshape(1536), slot2.reshape(1536)
    rows = pltpu.VMEM((1536, 128), F32)
    spread, fold, extra = kernel(
        second_body,
        (SMEM, SMEM, VMEM, VMEM, VMEM),
        (((EXT + 1024, 128), F32), ((32, 16, 128), F32), ((32, 128), F32)),
        (rows,),
    )(where, slot2, panels, mine, other)
    folds = lax.all_to_all(fold, "row", 0, 0, tiled=True)
    (own,) = kernel(first_body, (SMEM, VMEM), (((EXT, 128), F32),), (rows,))(slot1, panels)
    right, send0, send1 = kernel(
        image_body,
        (SMEM, SMEM, VMEM, VMEM, VMEM, ANY, VMEM, VMEM),
        (((EXT, 128), F32), ((64, 128), F32), ((64, 128), F32)),
        (rows, pltpu.VMEM((16, TALL, 256), F32), pltpu.SemaphoreType.DMA),
    )(where, slot1, folds, own, spread, blocks, extra, jnp.asarray(column_choice(), BF16))
    got0, got1 = transposed(send0, 0), transposed(send1, 1)
    left1, left2, share, own = kernel(
        cross_body,
        (SMEM, VMEM, VMEM, VMEM, VMEM),
        (((2, 9, 4, 128), F32), ((1, 9, 4, 128), F32), ((8, 72, 128), F32), ((16, 128), F32)),
    )(where, got0, got1, jnp.asarray(lane_order(), BF16), table)
    mine, other = along_cols(share)
    return kernel(
        diagonal_body,
        (SMEM,) + (VMEM,) * 9,
        (((2, 11, 4, 128), F32), ((1, 12, 4, 128), F32)),
    )(where, mine, other, right, spread, own, inverse_first, inverse_second, left1, left2)


def solution(mesh):
    tiles = P(None, None, "row", "col")
    panels = P("row", None, "col")
    return jax.shard_map(
        on_device,
        mesh=mesh,
        in_specs=(tiles, tiles, panels, P(), tiles, panels, P()),
        out_specs=(tiles, tiles),
        check_vma=False,
    )
```

```python
import jax
import jax.numpy as jnp
import numpy as np
from jax import lax
from jax.experimental import pallas as pl
from jax.experimental.pallas import tpu as pltpu
from jax.sharding import PartitionSpec as P


F32 = jnp.float32
BF16 = jnp.bfloat16
TALL = 144
SLOTS = 128
EXT = 16 * SLOTS

Y_GROUPS = [[4 * y + x for y in range(8)] for x in range(4)]
X_GROUPS = [[4 * y + x for x in range(4)] for y in range(8)]
Z_GROUPS = [[2 * z + k for z in range(8)] for k in range(2)]


def column_choice():
    table = np.zeros((96, 128), np.float32)
    for h in range(2):
        for m in range(32):
            al, k, q = m // 8, (m % 8) // 4, m % 4
            table[h * 48 + m, k * 32 + h * 16 + 4 * q + al] = 1
        for m in range(16):
            al, q = m // 4, m % 4
            table[h * 48 + 32 + m, 64 + h * 16 + 4 * q + al] = 1
    return table


def lane_order():
    table = np.zeros((512, 512), np.float32)
    for g in range(2):
        for al in range(4):
            for i in range(9):
                for q in range(4):
                    table[g * 256 + i * 16 + al * 4 + q, i * 32 + g * 16 + 4 * q + al] = 1
            for k in range(2):
                for q in range(4):
                    table[g * 256 + TALL + al * 8 + k * 4 + q, 384 + k * 32 + g * 16 + 4 * q + al] = 1
    return table


def dot(left, right):
    return jnp.dot(left, right, preferred_element_type=F32)


def halves(x):
    high = x.astype(BF16)
    return high, (x - high.astype(F32)).astype(BF16)


def thirds(x):
    high = x.astype(BF16)
    rest = x - high.astype(F32)
    mid = rest.astype(BF16)
    return high, mid, (rest - mid.astype(F32)).astype(BF16)


def product_terms(left, right):
    return dot(jnp.concatenate(halves(left), 0), jnp.concatenate(halves(right), 1))


def folded(terms):
    m, n = terms.shape[0] // 2, terms.shape[1] // 2
    return terms[:m, :n] + (terms[:m, n:] + terms[m:, :n])


def chosen(x, table):
    m = x.shape[0]
    out = dot(jnp.concatenate(thirds(x), 0), table)
    return out[:m] + (out[m : 2 * m] + out[2 * m :])


def lanes_of(shape):
    return lax.broadcasted_iota(jnp.int32, shape, len(shape) - 1)


def rank_body(s1, s2, tiles, packed, slot1, slot2, table, later, lhs, rhs, stage):
    col = lax.axis_index("col")
    upper = (
        lax.broadcasted_iota(jnp.int32, (128, 128), 0) < lax.broadcasted_iota(jnp.int32, (128, 128), 1)
    ).astype(BF16)
    groups = lax.broadcasted_iota(jnp.int32, (16, 128), 0)
    ranks = []
    count = jnp.zeros((8, 1), F32)
    listed = jnp.zeros((8, 384), F32)
    spot = lax.broadcasted_iota(jnp.int32, (384, 128), 0).astype(F32)
    kind = lax.broadcasted_iota(jnp.int32, (8, 128), 0)
    for which, (source, target) in enumerate(((s1, slot1), (s2, slot2))):
        carry = jnp.zeros((16, 1), F32)
        rank = []
        for m in range(12):
            row = source[m : m + 1, :]
            group = jnp.bitwise_and(lax.shift_right_logical(row, 5), 15)
            inside = row < 4608
            mark = ((group == groups) & inside).astype(F32)
            before = dot(mark.astype(BF16), upper) + carry
            t = jnp.sum(mark * before, axis=0, keepdims=True)
            carry = carry + jnp.sum(mark, axis=1, keepdims=True)
            rank.append(t + 1.0)
            place = group * SLOTS + t.astype(jnp.int32)
            if which:
                high = lax.shift_right_logical(row - 4608, 9)
                other = group * 64 + high * 32 + jnp.bitwise_and(row, 31)
                place = jnp.where(inside, place, EXT)
                mark = jnp.broadcast_to(jnp.where(inside, 0.0, 1.0), (8, 128))
                order = dot(mark.astype(BF16), upper) + count
                count = count + jnp.sum(mark, axis=1, keepdims=True)
                order = jnp.where(mark[0:1] > 0, order[0:1], -1.0)
                index = lanes_of((1, 128)) + m * 128
                value = jnp.where(kind == 0, lax.shift_right_logical(index, 6), jnp.bitwise_and(index, 63))
                value = jnp.where(kind == 2, lax.shift_right_logical(other, 6), value)
                value = jnp.where(kind == 3, jnp.bitwise_and(other, 63), value)
                value = jnp.where(kind == 4, 1, value)
                match = (order == spot).astype(BF16)
                listed = listed + lax.dot_general(
                    value.astype(F32).astype(BF16), match, (((1,), (1,)), ((), ())), preferred_element_type=F32
                )
            target[m : m + 1, :] = place
        ranks.append(rank)
    source_row = listed[0:1] * 64.0 + listed[1:2]
    target_row = jnp.where(listed[4:5] > 0.5, listed[2:3] * 64.0 + listed[3:4], 1024.0)
    later[...] = jnp.concatenate([source_row, target_row], 0).astype(jnp.int32)
    slots = lanes_of((32, 128)).astype(F32)
    table[288:, :] = jnp.zeros((96, 256), BF16)
    for j in range(9):
        spots = lax.broadcasted_iota(jnp.int32, (32, 128), 0) + (j * 512 + col * 32)
        both = []
        for source, rank in ((s1, ranks[0]), (s2, ranks[1])):
            total = jnp.zeros((32, 128), F32)
            for m in range(12):
                total = total + jnp.where(source[m : m + 1, :] == spots, rank[m], 0.0)
            slot = jnp.sum(total, axis=1, keepdims=True) - 1.0
            both.append((slot == slots).astype(BF16))
        pair = jnp.concatenate(both, 1)
        table[j * 32 : (j + 1) * 32, :] = pair
        for al in range(4):
            rhs[j * 128 + al * 32 : j * 128 + (al + 1) * 32, :] = pair
        quarter = lanes_of((4, 128)) // 32
        for i in range(9):
            for al in range(4):
                stage[i * 16 + al * 4 : i * 16 + (al + 1) * 4, :] = jnp.where(quarter == al, tiles[i, j], 0.0)
        for part, value in enumerate(thirds(stage[...])):
            lhs[part * TALL : (part + 1) * TALL, j * 128 : (j + 1) * 128] = value
    out = dot(lhs[...], rhs[...])
    packed[...] = out[:TALL] + (out[TALL : 2 * TALL] + out[2 * TALL :])


def lay_body(p1, p2, d1, panel, mixed, tall):
    tall[...] = jnp.zeros((128, 128), F32)
    tall[0:32, 0:48] = p1[0]
    tall[32:64, 0:48] = p1[1]
    tall[64:96, 0:48] = p2[0]
    both = tall[...].T[:48]
    lane = lanes_of((8, 128))
    spare = [jnp.where(lane < 96, 0.0, pltpu.roll(both[40:48], 96 - 32 * g, 1)) for g in range(3)]
    lane = lanes_of((40, 128))
    value = jnp.where(lane < 96, both[:40], jnp.concatenate([*spare, jnp.zeros((16, 128), F32)], 0))
    for n in range(8):
        panel[n] = value
    lane = lanes_of((4, 128))
    tall[0:48, :] = both
    for al in range(4):
        for k in range(2):
            value = jnp.zeros((4, 128), F32)
            for m in range(2):
                value = jnp.where(lane // 32 == m, pltpu.roll(d1[k, m], ((m - al) * 32) % 128, 1), value)
            tall[48 + al * 8 + k * 4 : 52 + al * 8 + k * 4, :] = value
    half = lanes_of((40, 128)) < 64
    value = jnp.where(half, tall[0:40, :], pltpu.roll(tall[40:80, :], 64, 1))
    for n in range(8):
        mixed[n] = value


def scatter_rows(slots, source, target):
    def place(step, _):
        base = pl.multiple_of(step * 48, 16)
        for u in range(48):
            target[pl.ds(slots[base + u], 1), :] = source[pl.ds(base + u, 1), :]
        return 0

    lax.fori_loop(0, 32, place, 0)


def in_order(step):
    return ((step % 8) * 4 + step // 8) * 48


def opened(panels, step):
    piece = panels[step // 8, step % 8]
    lane = lanes_of((8, 128))
    tail = pltpu.roll(piece[16:24], 96, 1)
    tail = jnp.where(lane < 64, pltpu.roll(piece[8:16], 64, 1), tail)
    tail = jnp.where(lane < 32, pltpu.roll(piece[0:8], 32, 1), tail)
    return jnp.concatenate([piece, tail], 0)


def second_body(later, panels, mine, other, spread, fold, extra, rows):
    lane = lanes_of((48, 128))
    keep = (lane >= 64) & (lane < 96)

    def copy(step):
        rows[pl.ds(in_order(step), 48), :] = jnp.where(keep, opened(panels, step), 0.0)
        return 0

    for step in range(32):
        copy(step)
    spread[...] = jnp.zeros(spread.shape, F32)

    def place(step, _):
        for u in range(48):
            n = step * 48 + u
            spread[pl.ds(later[1, n], 1), :] = rows[pl.ds(later[0, n], 1), :]
        return 0

    lax.fori_loop(0, 8, place, 0)
    core = lax.axis_index("col") % 2
    half = lanes_of((40, 128)) < 64
    total = jnp.zeros((160, 256), F32)
    for z in range(8):
        for source, k in ((mine, core), (other, 1 - core)):
            x = source[z]
            left = jnp.concatenate([jnp.where(half, x, 0.0), jnp.where(half, 0.0, x)], 0)
            right = spread[pl.ds(pl.multiple_of((2 * z + k) * 64, 64), 64), :]
            total = total + product_terms(left, jnp.concatenate([right, right], 0))
    out = folded(total)
    lane_f = lanes_of((16, 128))
    value = jnp.zeros((16, 128), F32)
    for h in range(3):
        moved = pltpu.roll(out[16 * h : 16 * (h + 1), :], (32 * h - 64) % 128, 1)
        value = jnp.where(lane_f // 32 == h, moved, value)
    for n in range(32):
        fold[n] = value
    extra[...] = out[48:80, :]


def first_body(slot1, slot2, panels, own, spread, rows1, rows2):
    lane = lanes_of((48, 128))

    def copy(step):
        value = opened(panels, step)
        rows1[pl.ds(in_order(step), 48), :] = jnp.where(lane < 64, value, 0.0)
        rows2[pl.ds(in_order(step), 48), :] = jnp.where((lane >= 64) & (lane < 96), value, 0.0)
        return 0

    for step in range(32):
        copy(step)
    own[...] = jnp.zeros(own.shape, F32)
    spread[...] = jnp.zeros(spread.shape, F32)

    def place(step, _):
        base = pl.multiple_of(step * 48, 16)
        for u in range(48):
            own[pl.ds(slot1[base + u], 1), :] = rows1[pl.ds(base + u, 1), :]
            spread[pl.ds(slot2[base + u], 1), :] = rows2[pl.ds(base + u, 1), :]
        return 0

    lax.fori_loop(0, 32, place, 0)


def image_body(slot1, fold, own, second, blocks, extra, choice, right, send0, send1, rows, held, done):
    send = (send0, send1)
    arrival = pltpu.make_async_copy(blocks, held, done)
    arrival.start()
    keep = lanes_of((16, 128))
    keep = (keep >= 64) & (keep < 96)

    def join(step):
        q = -fold[step]
        base = step * 48
        for h in range(3):
            moved = pltpu.roll(q, (64 - 32 * h) % 128, 1)
            rows[pl.ds(base + 16 * h, 16), :] = jnp.where(keep, moved, 0.0)
        return 0

    for step in range(32):
        join(step)
    right[...] = jnp.zeros(right.shape, F32)
    scatter_rows(slot1, rows, right)
    right[...] = right[...] + own[...]
    arrival.wait()
    total = jnp.zeros((2 * TALL, 256), F32)
    for c in range(16):
        part = slice(c * SLOTS, (c + 1) * SLOTS)
        total = total + product_terms(held[c], jnp.concatenate([right[part, :], second[part, :]], 0))
    image = jnp.concatenate([folded(total), extra[...]], 0)
    sent = jnp.zeros((96, TALL + 32), F32)
    for part in thirds(image):
        sent = sent + lax.dot_general(choice[...], part, (((1,), (1,)), ((), ())), preferred_element_type=F32)
    lane = lanes_of((16, 128))
    pieces = []
    for h in range(2):
        rest = jnp.concatenate([sent[h * 48 : (h + 1) * 48, 128:], jnp.zeros((48, 80), F32)], 1)
        tail = jnp.where(lane < 16, rest[0:16], pltpu.roll(rest[16:32], 16, 1))
        tail = jnp.where(lane < 32, tail, pltpu.roll(rest[32:48], 32, 1))
        pieces.append(jnp.concatenate([sent[h * 48 : (h + 1) * 48, :128], tail], 0))
    parity = lax.axis_index("row") % 2
    for h in range(2):

        @pl.when(parity == h)
        def _(h=h):
            send[0][...] = pieces[h]
            send[1][...] = pieces[1 - h]


def cross_body(got0, got1, order, table, first, second, share, own):
    parity = lax.axis_index("row") % 2
    a, b = got0[...], got1[...]
    even = jnp.where(parity == 0, a, b)
    odd = jnp.where(parity == 0, b, a)
    parts = []
    for got in (even, odd):
        tail = got[48:64]
        parts.append(got[:48])
        parts.append(jnp.concatenate([tail, pltpu.roll(tail, 112, 1), pltpu.roll(tail, 96, 1)], 0))
    y = chosen(jnp.concatenate(parts, 1), order[...])
    close = chosen(y[:, :384], table[...])
    e = y[32:48, 384:512]
    own[...] = e
    lane = lanes_of((8, 128))
    e = jnp.where(lane < 64, e[:8], pltpu.roll(e[8:], 64, 1))
    e = jnp.concatenate([close[:, :128], close[32:48, 128:], e], 0)
    for n in range(8):
        share[n] = e
    lane2 = lanes_of((4, 128))
    for i in range(9):
        chunk = (i // 4) * 128
        one = jnp.zeros((8, 128), F32)
        two = jnp.zeros((4, 128), F32)
        for al in range(4):
            shift = ((al - i % 4) * 32) % 128
            moved = pltpu.roll(y[al * 8 : (al + 1) * 8, chunk : chunk + 128], shift, 1) if shift else y[al * 8 : (al + 1) * 8, chunk : chunk + 128]
            one = jnp.where(lane // 32 == al, moved, one)
            low = y[32 + al * 4 : 36 + al * 4, chunk : chunk + 128]
            moved = pltpu.roll(low, shift, 1) if shift else low
            two = jnp.where(lane2 // 32 == al, moved, two)
        first[0, i] = -one[0:4]
        first[1, i] = -one[4:8]
        second[0, i] = -two


def diagonal_body(mine, other, right, spread, later, own, d1, d2, left1, left2, first, second):
    first[:, 0:9] = left1[...]
    second[:, 0:9] = left2[...]
    core = lax.axis_index("col") % 2
    lane_e = lanes_of((8, 128))
    total = jnp.zeros((128, 256), F32)
    also = jnp.zeros((32, 256), F32)
    for z in range(8):
        for source, k in ((mine, core), (other, 1 - core)):
            c = 2 * z + k
            x = source[z]
            part = pl.ds(pl.multiple_of(c * SLOTS, SLOTS), SLOTS)
            zero = jnp.zeros((48, 128), F32)
            left = jnp.concatenate(
                [jnp.concatenate([x[:48], zero], 1), jnp.concatenate([zero[:16], x[48:64]], 1)], 0
            )
            total = total + product_terms(left, jnp.concatenate([right[part, :], spread[part, :]], 0))
            e = x[64:72]
            left = jnp.concatenate([jnp.where(lane_e < 64, e, 0.0), jnp.where(lane_e >= 64, e, 0.0)], 0)
            v = later[pl.ds(pl.multiple_of(c * 64, 64), 64), :]
            also = also + product_terms(left, jnp.concatenate([v, v], 0))
    out = folded(total)
    g1 = out[:32]
    bottom = own[...] - out[32:48]
    g2 = out[32:48] + out[48:64] + folded(also)
    lane = lanes_of((8, 128))
    lane2 = lanes_of((4, 128))
    for k in range(2):
        one = jnp.zeros((8, 128), F32)
        two = jnp.zeros((4, 128), F32)
        for al in range(4):
            shift = ((al - k) * 32) % 128
            one = jnp.where(lane // 32 == al, pltpu.roll(g1[al * 8 : (al + 1) * 8], shift, 1), one)
            two = jnp.where(lane2 // 32 == al, pltpu.roll(bottom[al * 4 : (al + 1) * 4], shift, 1), two)
        first[0, 9 + k] = d1[0, k] + one[0:4]
        first[1, 9 + k] = d1[1, k] + one[4:8]
        second[0, 9 + k] = -two
    two = jnp.zeros((4, 128), F32)
    for al in range(4):
        shift = ((al - 2) * 32) % 128
        two = jnp.where(lane2 // 32 == al, pltpu.roll(g2[al * 4 : (al + 1) * 4], shift, 1), two)
    second[0, 11] = d2[0, 0] + two


VMEM = pl.BlockSpec(memory_space=pltpu.VMEM)
SMEM = pl.BlockSpec(memory_space=pltpu.SMEM)
ANY = pl.BlockSpec(memory_space=pl.ANY)


def kernel(body, specs, outs, scratch=()):
    return pl.pallas_call(
        body,
        in_specs=list(specs),
        out_specs=[VMEM] * len(outs),
        out_shape=[jax.ShapeDtypeStruct(shape, dtype) for shape, dtype in outs],
        scratch_shapes=list(scratch),
    )


def exchanged(x, axis, groups):
    return lax.all_to_all(x, axis, 0, 0, axis_index_groups=groups, tiled=True)


def along_rows(x):
    near = exchanged(x, "row", Y_GROUPS)
    return exchanged(jnp.broadcast_to(near, (4, *near.shape)), "row", X_GROUPS)


def swapped(x):
    return lax.ppermute(x, "col", [(c, c ^ 1) for c in range(16)])


def transposed(x, turn):
    pairs = [(r * 16 + c, (2 * c + (r + turn) % 2) * 16 + r // 2) for r in range(32) for c in range(16)]
    return lax.ppermute(x, ("row", "col"), pairs)


def on_device(ancestor, inverse_first, panel_first, structure_first, inverse_second, panel_second, structure_second):
    panel, mixed = kernel(
        lay_body,
        (VMEM, VMEM, VMEM),
        (((8, 40, 128), F32), ((8, 40, 128), F32)),
        (pltpu.VMEM((128, 128), F32),),
    )(panel_first.transpose(1, 2, 0), panel_second.transpose(1, 2, 0), inverse_first)
    packed, slot1, slot2, table, later = kernel(
        rank_body,
        (VMEM, VMEM, VMEM),
        (((TALL, 256), F32), ((12, 128), jnp.int32), ((12, 128), jnp.int32), ((384, 256), BF16), ((2, 384), jnp.int32)),
        (pltpu.VMEM((3 * TALL, 1152), BF16), pltpu.VMEM((1152, 256), BF16), pltpu.VMEM((TALL, 128), F32)),
    )(structure_first.reshape(12, 128), structure_second.reshape(12, 128), ancestor)
    blocks = lax.all_gather(packed, "col")
    mine = exchanged(mixed, "col", Z_GROUPS)
    other = swapped(mine)
    panels = along_rows(panel)
    slot1, slot2 = slot1.reshape(1536), slot2.reshape(1536)
    rows = pltpu.VMEM((1536, 128), F32)
    second, fold, extra = kernel(
        second_body,
        (SMEM, VMEM, VMEM, VMEM),
        (((1032, 128), F32), ((32, 16, 128), F32), ((32, 128), F32)),
        (rows,),
    )(later, panels, mine, other)
    folds = lax.all_to_all(fold, "row", 0, 0, tiled=True)
    own, spread = kernel(
        first_body, (SMEM, SMEM, VMEM), (((EXT, 128), F32), ((EXT + 8, 128), F32)), (rows, rows)
    )(slot1, slot2, panels)
    right, send0, send1 = kernel(
        image_body,
        (SMEM, VMEM, VMEM, VMEM, ANY, VMEM, VMEM),
        (((EXT, 128), F32), ((64, 128), F32), ((64, 128), F32)),
        (rows, pltpu.VMEM((16, TALL, 256), F32), pltpu.SemaphoreType.DMA),
    )(slot1, folds, own, spread, blocks, extra, jnp.asarray(column_choice(), BF16))
    got0, got1 = transposed(send0, 0), transposed(send1, 1)
    left1, left2, share, own = kernel(
        cross_body,
        (VMEM, VMEM, VMEM, VMEM),
        (((2, 9, 4, 128), F32), ((1, 9, 4, 128), F32), ((8, 72, 128), F32), ((16, 128), F32)),
    )(got0, got1, jnp.asarray(lane_order(), BF16), table)
    mine = exchanged(share, "col", Z_GROUPS)
    other = swapped(mine)
    return kernel(
        diagonal_body,
        (VMEM,) * 10,
        (((2, 11, 4, 128), F32), ((1, 12, 4, 128), F32)),
    )(mine, other, right, spread, second, own, inverse_first, inverse_second, left1, left2)


def solution(mesh):
    tiles = P(None, None, "row", "col")
    panels = P("row", None, "col")

    return jax.shard_map(
        on_device,
        mesh=mesh,
        in_specs=(tiles, tiles, panels, P(), tiles, panels, P()),
        out_specs=(tiles, tiles),
        check_vma=False,
    )
```

```python
import jax
import jax.numpy as jnp
import numpy as np
from jax import lax
from jax.experimental import pallas as pl
from jax.experimental.pallas import tpu as pltpu
from jax.sharding import PartitionSpec as P


F32 = jnp.float32
BF16 = jnp.bfloat16
TALL = 144
SLOTS = 128
EXT = 16 * SLOTS

Y_GROUPS = [[4 * y + x for y in range(8)] for x in range(4)]
X_GROUPS = [[4 * y + x for x in range(4)] for y in range(8)]
Z_GROUPS = [[2 * z + k for z in range(8)] for k in range(2)]


def column_choice():
    table = np.zeros((96, 128), np.float32)
    for h in range(2):
        for m in range(32):
            al, k, q = m // 8, (m % 8) // 4, m % 4
            table[h * 48 + m, k * 32 + h * 16 + 4 * q + al] = 1
        for m in range(16):
            al, q = m // 4, m % 4
            table[h * 48 + 32 + m, 64 + h * 16 + 4 * q + al] = 1
    return table


def lane_order():
    table = np.zeros((512, 512), np.float32)
    for g in range(2):
        for al in range(4):
            for i in range(9):
                for q in range(4):
                    table[g * 256 + i * 16 + al * 4 + q, i * 32 + g * 16 + 4 * q + al] = 1
            for k in range(2):
                for q in range(4):
                    table[g * 256 + TALL + al * 8 + k * 4 + q, 384 + k * 32 + g * 16 + 4 * q + al] = 1
    return table


def dot(left, right):
    return jnp.dot(left, right, preferred_element_type=F32)


def halves(x):
    high = x.astype(BF16)
    return high, (x - high.astype(F32)).astype(BF16)


def thirds(x):
    high = x.astype(BF16)
    rest = x - high.astype(F32)
    mid = rest.astype(BF16)
    return high, mid, (rest - mid.astype(F32)).astype(BF16)


def product_terms(left, right):
    return dot(jnp.concatenate(halves(left), 0), jnp.concatenate(halves(right), 1))


def folded(terms):
    m, n = terms.shape[0] // 2, terms.shape[1] // 2
    return terms[:m, :n] + (terms[:m, n:] + terms[m:, :n])


def chosen(x, table):
    m = x.shape[0]
    out = dot(jnp.concatenate(thirds(x), 0), table)
    return out[:m] + (out[m : 2 * m] + out[2 * m :])


def lanes_of(shape):
    return lax.broadcasted_iota(jnp.int32, shape, len(shape) - 1)


def rank_body(s1, s2, tiles, packed, slot1, slot2, table, later, lhs, rhs, stage):
    col = lax.axis_index("col")
    upper = (
        lax.broadcasted_iota(jnp.int32, (128, 128), 0) < lax.broadcasted_iota(jnp.int32, (128, 128), 1)
    ).astype(BF16)
    groups = lax.broadcasted_iota(jnp.int32, (16, 128), 0)
    ranks = []
    count = jnp.zeros((8, 1), F32)
    listed = jnp.zeros((8, 384), F32)
    spot = lax.broadcasted_iota(jnp.int32, (384, 128), 0).astype(F32)
    kind = lax.broadcasted_iota(jnp.int32, (8, 128), 0)
    for which, (source, target) in enumerate(((s1, slot1), (s2, slot2))):
        carry = jnp.zeros((16, 1), F32)
        rank = []
        for m in range(12):
            row = source[m : m + 1, :]
            group = jnp.bitwise_and(lax.shift_right_logical(row, 5), 15)
            inside = row < 4608
            mark = ((group == groups) & inside).astype(F32)
            before = dot(mark.astype(BF16), upper) + carry
            t = jnp.sum(mark * before, axis=0, keepdims=True)
            carry = carry + jnp.sum(mark, axis=1, keepdims=True)
            rank.append(t + 1.0)
            place = group * SLOTS + t.astype(jnp.int32)
            if which:
                high = lax.shift_right_logical(row - 4608, 9)
                other = group * 64 + high * 32 + jnp.bitwise_and(row, 31)
                place = jnp.where(inside, place, EXT)
                mark = jnp.broadcast_to(jnp.where(inside, 0.0, 1.0), (8, 128))
                order = dot(mark.astype(BF16), upper) + count
                count = count + jnp.sum(mark, axis=1, keepdims=True)
                order = jnp.where(mark[0:1] > 0, order[0:1], -1.0)
                index = lanes_of((1, 128)) + m * 128
                value = jnp.where(kind == 0, lax.shift_right_logical(index, 6), jnp.bitwise_and(index, 63))
                value = jnp.where(kind == 2, lax.shift_right_logical(other, 6), value)
                value = jnp.where(kind == 3, jnp.bitwise_and(other, 63), value)
                value = jnp.where(kind == 4, 1, value)
                match = (order == spot).astype(BF16)
                listed = listed + lax.dot_general(
                    value.astype(F32).astype(BF16), match, (((1,), (1,)), ((), ())), preferred_element_type=F32
                )
            target[m : m + 1, :] = place
        ranks.append(rank)
    source_row = listed[0:1] * 64.0 + listed[1:2]
    target_row = jnp.where(listed[4:5] > 0.5, listed[2:3] * 64.0 + listed[3:4], 1024.0)
    later[...] = jnp.concatenate([source_row, target_row], 0).astype(jnp.int32)
    slots = lanes_of((32, 128)).astype(F32)
    table[288:, :] = jnp.zeros((96, 256), BF16)
    for j in range(9):
        spots = lax.broadcasted_iota(jnp.int32, (32, 128), 0) + (j * 512 + col * 32)
        both = []
        for source, rank in ((s1, ranks[0]), (s2, ranks[1])):
            total = jnp.zeros((32, 128), F32)
            for m in range(12):
                total = total + jnp.where(source[m : m + 1, :] == spots, rank[m], 0.0)
            slot = jnp.sum(total, axis=1, keepdims=True) - 1.0
            both.append((slot == slots).astype(BF16))
        pair = jnp.concatenate(both, 1)
        table[j * 32 : (j + 1) * 32, :] = pair
        for al in range(4):
            rhs[j * 128 + al * 32 : j * 128 + (al + 1) * 32, :] = pair
        quarter = lanes_of((4, 128)) // 32
        for i in range(9):
            for al in range(4):
                stage[i * 16 + al * 4 : i * 16 + (al + 1) * 4, :] = jnp.where(quarter == al, tiles[i, j], 0.0)
        for part, value in enumerate(thirds(stage[...])):
            lhs[part * TALL : (part + 1) * TALL, j * 128 : (j + 1) * 128] = value
    out = dot(lhs[...], rhs[...])
    packed[...] = out[:TALL] + (out[TALL : 2 * TALL] + out[2 * TALL :])


def lay_body(p1, p2, d1, panel, near, mixed, tall):
    tall[...] = jnp.zeros((128, 128), F32)
    tall[0:32, 0:48] = p1[0]
    tall[32:64, 0:48] = p1[1]
    tall[64:96, 0:48] = p2[0]
    both = tall[...].T[:48]
    lane = lanes_of((16, 128))
    value = jnp.zeros((16, 128), F32)
    for h in range(3):
        moved = pltpu.roll(both[16 * h : 16 * (h + 1)], (32 * h - 64) % 128, 1)
        value = jnp.where(lane // 32 == h, moved, value)
    for n in range(32):
        panel[n] = value
    near[...] = jnp.where(lanes_of((24, 128)) < 64, both[:24], pltpu.roll(both[24:], 64, 1))
    lane = lanes_of((4, 128))
    tall[0:48, :] = both
    for al in range(4):
        for k in range(2):
            value = jnp.zeros((4, 128), F32)
            for m in range(2):
                value = jnp.where(lane // 32 == m, pltpu.roll(d1[k, m], ((m - al) * 32) % 128, 1), value)
            tall[48 + al * 8 + k * 4 : 52 + al * 8 + k * 4, :] = value
    half = lanes_of((40, 128)) < 64
    value = jnp.where(half, tall[0:40, :], pltpu.roll(tall[40:80, :], 64, 1))
    for n in range(8):
        mixed[n] = value


def scatter_rows(slots, source, target):
    def place(step, _):
        base = pl.multiple_of(step * 48, 16)
        for u in range(48):
            target[pl.ds(slots[base + u], 1), :] = source[pl.ds(base + u, 1), :]
        return 0

    lax.fori_loop(0, 32, place, 0)


def in_order(step):
    return ((step % 8) * 4 + step // 8) * 48


def unfold(folds, rows):
    keep = lanes_of((16, 128))
    keep = (keep >= 64) & (keep < 96)
    for r in range(32):
        for h in range(3):
            moved = pltpu.roll(folds[r], (64 - 32 * h) % 128, 1)
            rows[r * 48 + 16 * h : r * 48 + 16 * (h + 1), :] = jnp.where(keep, moved, 0.0)


def second_body(later, panels, near, mine, other, spread, fold, extra, rows):
    unfold(panels, rows)
    spread[...] = jnp.zeros(spread.shape, F32)

    def place(step, _):
        for u in range(48):
            n = step * 48 + u
            spread[pl.ds(later[1, n], 1), :] = rows[pl.ds(later[0, n], 1), :]
        return 0

    lax.fori_loop(0, 8, place, 0)
    core = lax.axis_index("col") % 2
    half = lanes_of((40, 128)) < 64
    total = jnp.zeros((160, 256), F32)
    for z in range(8):
        for source, k in ((mine, core), (other, 1 - core)):
            x = source[z]
            left = jnp.concatenate([jnp.where(half, x, 0.0), jnp.where(half, 0.0, x)], 0)
            right = spread[pl.ds(pl.multiple_of((2 * z + k) * 64, 64), 64), :]
            total = total + product_terms(left, jnp.concatenate([right, right], 0))
    out = folded(total)
    lane_f = lanes_of((16, 128))
    value = jnp.zeros((16, 128), F32)
    for h in range(3):
        moved = pltpu.roll(out[16 * h : 16 * (h + 1), :], (32 * h - 64) % 128, 1)
        value = jnp.where(lane_f // 32 == h, moved, value)
    value = jnp.concatenate([value, near[...]], 0)
    for n in range(8):
        fold[n] = value
    extra[...] = out[48:80, :]


def first_body(slot2, panels, spread, rows):
    unfold(panels, rows)
    spread[...] = jnp.zeros(spread.shape, F32)
    scatter_rows(slot2, rows, spread)


def image_body(slot1, folds, second_hbm, blocks, extra, choice, out, send0, send1, rows, held, second, right, done):
    send = (send0, send1)
    third = pltpu.make_async_copy(second_hbm.at[pl.ds(0, EXT)], second, done.at[0])
    arrival = pltpu.make_async_copy(blocks, held, done.at[1])
    leaving = pltpu.make_async_copy(right, out, done.at[2])
    third.start()
    arrival.start()
    lane = lanes_of((16, 128))
    for step in range(32):
        piece = folds[step // 8, step % 8]
        base = in_order(step)
        near = jnp.concatenate([piece[16:], pltpu.roll(piece[16:], 64, 1)], 0)
        for h in range(3):
            moved = jnp.where(lane < 96, -pltpu.roll(piece[:16], (64 - 32 * h) % 128, 1), 0.0)
            rows[base + 16 * h : base + 16 * (h + 1), :] = jnp.where(lane < 64, near[16 * h : 16 * (h + 1)], moved)
    right[...] = jnp.zeros(right.shape, F32)
    scatter_rows(slot1, rows, right)
    leaving.start()
    third.wait()
    arrival.wait()
    total = jnp.zeros((2 * TALL, 256), F32)
    for c in range(16):
        part = slice(c * SLOTS, (c + 1) * SLOTS)
        total = total + product_terms(held[c], jnp.concatenate([right[part, :], second[part, :]], 0))
    image = jnp.concatenate([folded(total), extra[...]], 0)
    sent = jnp.zeros((96, TALL + 32), F32)
    for part in thirds(image):
        sent = sent + lax.dot_general(choice[...], part, (((1,), (1,)), ((), ())), preferred_element_type=F32)
    lane = lanes_of((16, 128))
    pieces = []
    for h in range(2):
        rest = jnp.concatenate([sent[h * 48 : (h + 1) * 48, 128:], jnp.zeros((48, 80), F32)], 1)
        tail = jnp.where(lane < 16, rest[0:16], pltpu.roll(rest[16:32], 16, 1))
        tail = jnp.where(lane < 32, tail, pltpu.roll(rest[32:48], 32, 1))
        pieces.append(jnp.concatenate([sent[h * 48 : (h + 1) * 48, :128], tail], 0))
    parity = lax.axis_index("row") % 2
    for h in range(2):

        @pl.when(parity == h)
        def _(h=h):
            send[0][...] = pieces[h]
            send[1][...] = pieces[1 - h]

    leaving.wait()


def cross_body(got0, got1, order, table, first, second, share, own):
    parity = lax.axis_index("row") % 2
    a, b = got0[...], got1[...]
    even = jnp.where(parity == 0, a, b)
    odd = jnp.where(parity == 0, b, a)
    parts = []
    for got in (even, odd):
        tail = got[48:64]
        parts.append(got[:48])
        parts.append(jnp.concatenate([tail, pltpu.roll(tail, 112, 1), pltpu.roll(tail, 96, 1)], 0))
    y = chosen(jnp.concatenate(parts, 1), order[...])
    close = chosen(y[:, :384], table[...])
    e = y[32:48, 384:512]
    own[...] = e
    lane = lanes_of((8, 128))
    e = jnp.where(lane < 64, e[:8], pltpu.roll(e[8:], 64, 1))
    e = jnp.concatenate([close[:, :128], close[32:48, 128:], e], 0)
    for n in range(8):
        share[n] = e
    lane2 = lanes_of((4, 128))
    for i in range(9):
        chunk = (i // 4) * 128
        one = jnp.zeros((8, 128), F32)
        two = jnp.zeros((4, 128), F32)
        for al in range(4):
            shift = ((al - i % 4) * 32) % 128
            moved = pltpu.roll(y[al * 8 : (al + 1) * 8, chunk : chunk + 128], shift, 1) if shift else y[al * 8 : (al + 1) * 8, chunk : chunk + 128]
            one = jnp.where(lane // 32 == al, moved, one)
            low = y[32 + al * 4 : 36 + al * 4, chunk : chunk + 128]
            moved = pltpu.roll(low, shift, 1) if shift else low
            two = jnp.where(lane2 // 32 == al, moved, two)
        first[0, i] = -one[0:4]
        first[1, i] = -one[4:8]
        second[0, i] = -two


def diagonal_body(mine, other, right, spread, later, own, d1, d2, left1, left2, first, second):
    first[:, 0:9] = left1[...]
    second[:, 0:9] = left2[...]
    core = lax.axis_index("col") % 2
    lane_e = lanes_of((8, 128))
    total = jnp.zeros((128, 256), F32)
    also = jnp.zeros((32, 256), F32)
    for z in range(8):
        for source, k in ((mine, core), (other, 1 - core)):
            c = 2 * z + k
            x = source[z]
            part = pl.ds(pl.multiple_of(c * SLOTS, SLOTS), SLOTS)
            zero = jnp.zeros((48, 128), F32)
            left = jnp.concatenate(
                [jnp.concatenate([x[:48], zero], 1), jnp.concatenate([zero[:16], x[48:64]], 1)], 0
            )
            total = total + product_terms(left, jnp.concatenate([right[part, :], spread[part, :]], 0))
            e = x[64:72]
            left = jnp.concatenate([jnp.where(lane_e < 64, e, 0.0), jnp.where(lane_e >= 64, e, 0.0)], 0)
            v = later[pl.ds(pl.multiple_of(c * 64, 64), 64), :]
            also = also + product_terms(left, jnp.concatenate([v, v], 0))
    out = folded(total)
    g1 = out[:32]
    bottom = own[...] - out[32:48]
    g2 = out[32:48] + out[48:64] + folded(also)
    lane = lanes_of((8, 128))
    lane2 = lanes_of((4, 128))
    for k in range(2):
        one = jnp.zeros((8, 128), F32)
        two = jnp.zeros((4, 128), F32)
        for al in range(4):
            shift = ((al - k) * 32) % 128
            one = jnp.where(lane // 32 == al, pltpu.roll(g1[al * 8 : (al + 1) * 8], shift, 1), one)
            two = jnp.where(lane2 // 32 == al, pltpu.roll(bottom[al * 4 : (al + 1) * 4], shift, 1), two)
        first[0, 9 + k] = d1[0, k] + one[0:4]
        first[1, 9 + k] = d1[1, k] + one[4:8]
        second[0, 9 + k] = -two
    two = jnp.zeros((4, 128), F32)
    for al in range(4):
        shift = ((al - 2) * 32) % 128
        two = jnp.where(lane2 // 32 == al, pltpu.roll(g2[al * 4 : (al + 1) * 4], shift, 1), two)
    second[0, 11] = d2[0, 0] + two


VMEM = pl.BlockSpec(memory_space=pltpu.VMEM)
SMEM = pl.BlockSpec(memory_space=pltpu.SMEM)
ANY = pl.BlockSpec(memory_space=pl.ANY)


def kernel(body, specs, outs, scratch=(), places=None):
    return pl.pallas_call(
        body,
        in_specs=list(specs),
        out_specs=list(places or [VMEM] * len(outs)),
        out_shape=[jax.ShapeDtypeStruct(shape, dtype) for shape, dtype in outs],
        scratch_shapes=list(scratch),
    )


def exchanged(x, axis, groups):
    return lax.all_to_all(x, axis, 0, 0, axis_index_groups=groups, tiled=True)


def swapped(x):
    return lax.ppermute(x, "col", [(c, c ^ 1) for c in range(16)])


def transposed(x, turn):
    pairs = [(r * 16 + c, (2 * c + (r + turn) % 2) * 16 + r // 2) for r in range(32) for c in range(16)]
    return lax.ppermute(x, ("row", "col"), pairs)


def on_device(ancestor, inverse_first, panel_first, structure_first, inverse_second, panel_second, structure_second):
    panel, near, mixed = kernel(
        lay_body,
        (VMEM, VMEM, VMEM),
        (((32, 16, 128), F32), ((24, 128), F32), ((8, 40, 128), F32)),
        (pltpu.VMEM((128, 128), F32),),
    )(panel_first.transpose(1, 2, 0), panel_second.transpose(1, 2, 0), inverse_first)
    packed, slot1, slot2, table, later = kernel(
        rank_body,
        (VMEM, VMEM, VMEM),
        (((TALL, 256), F32), ((12, 128), jnp.int32), ((12, 128), jnp.int32), ((384, 256), BF16), ((2, 384), jnp.int32)),
        (pltpu.VMEM((3 * TALL, 1152), BF16), pltpu.VMEM((1152, 256), BF16), pltpu.VMEM((TALL, 128), F32)),
    )(structure_first.reshape(12, 128), structure_second.reshape(12, 128), ancestor)
    blocks = lax.all_gather(packed, "col")
    mine = exchanged(mixed, "col", Z_GROUPS)
    other = swapped(mine)
    panels = lax.all_to_all(panel, "row", 0, 0, tiled=True)
    slot1, slot2 = slot1.reshape(1536), slot2.reshape(1536)
    rows = pltpu.VMEM((1536, 128), F32)
    second, fold, extra = kernel(
        second_body,
        (SMEM, VMEM, VMEM, VMEM, VMEM),
        (((1032, 128), F32), ((8, 40, 128), F32), ((32, 128), F32)),
        (rows,),
    )(later, panels, near, mine, other)
    folds = exchanged(fold, "row", Y_GROUPS)
    folds = exchanged(jnp.broadcast_to(folds, (4, *folds.shape)), "row", X_GROUPS)
    (spread,) = kernel(first_body, (SMEM, VMEM), (((EXT + 8, 128), F32),), (rows,))(slot2, panels)
    big = pltpu.VMEM((EXT, 128), F32)
    right, send0, send1 = kernel(
        image_body,
        (SMEM, VMEM, ANY, ANY, VMEM, VMEM),
        (((EXT, 128), F32), ((64, 128), F32), ((64, 128), F32)),
        (rows, pltpu.VMEM((16, TALL, 256), F32), big, big, pltpu.SemaphoreType.DMA((3,))),
        (ANY, VMEM, VMEM),
    )(slot1, folds, spread, blocks, extra, jnp.asarray(column_choice(), BF16))
    got0, got1 = transposed(send0, 0), transposed(send1, 1)
    left1, left2, share, own = kernel(
        cross_body,
        (VMEM, VMEM, VMEM, VMEM),
        (((2, 9, 4, 128), F32), ((1, 9, 4, 128), F32), ((8, 72, 128), F32), ((16, 128), F32)),
    )(got0, got1, jnp.asarray(lane_order(), BF16), table)
    mine = exchanged(share, "col", Z_GROUPS)
    other = swapped(mine)
    return kernel(
        diagonal_body,
        (VMEM,) * 10,
        (((2, 11, 4, 128), F32), ((1, 12, 4, 128), F32)),
    )(mine, other, right, spread, second, own, inverse_first, inverse_second, left1, left2)


def solution(mesh):
    tiles = P(None, None, "row", "col")
    panels = P("row", None, "col")

    return jax.shard_map(
        on_device,
        mesh=mesh,
        in_specs=(tiles, tiles, panels, P(), tiles, panels, P()),
        out_specs=(tiles, tiles),
        check_vma=False,
    )
```

```python
import jax
import jax.numpy as jnp
import numpy as np
from jax import lax
from jax.experimental import pallas as pl
from jax.experimental.pallas import tpu as pltpu
from jax.sharding import PartitionSpec as P


F32 = jnp.float32
BF16 = jnp.bfloat16
TALL = 144
SLOTS = 128
EXT = 16 * SLOTS

Y_GROUPS = [[4 * y + x for y in range(8)] for x in range(4)]
X_GROUPS = [[4 * y + x for x in range(4)] for y in range(8)]
Z_GROUPS = [[2 * z + k for z in range(8)] for k in range(2)]


def column_choice():
    table = np.zeros((96, 128), np.float32)
    for h in range(2):
        for m in range(32):
            al, k, q = m // 8, (m % 8) // 4, m % 4
            table[h * 48 + m, k * 32 + h * 16 + 4 * q + al] = 1
        for m in range(16):
            al, q = m // 4, m % 4
            table[h * 48 + 32 + m, 64 + h * 16 + 4 * q + al] = 1
    return table


def lane_order():
    table = np.zeros((512, 512), np.float32)
    for g in range(2):
        for al in range(4):
            for i in range(9):
                for q in range(4):
                    table[g * 256 + i * 16 + al * 4 + q, i * 32 + g * 16 + 4 * q + al] = 1
            for k in range(2):
                for q in range(4):
                    table[g * 256 + TALL + al * 8 + k * 4 + q, 384 + k * 32 + g * 16 + 4 * q + al] = 1
    return table


def dot(left, right):
    return jnp.dot(left, right, preferred_element_type=F32)


def halves(x):
    high = x.astype(BF16)
    return high, (x - high.astype(F32)).astype(BF16)


def thirds(x):
    high = x.astype(BF16)
    rest = x - high.astype(F32)
    mid = rest.astype(BF16)
    return high, mid, (rest - mid.astype(F32)).astype(BF16)


def product_terms(left, right):
    return dot(jnp.concatenate(halves(left), 0), jnp.concatenate(halves(right), 1))


def folded(terms):
    m, n = terms.shape[0] // 2, terms.shape[1] // 2
    return terms[:m, :n] + (terms[:m, n:] + terms[m:, :n])


def chosen(x, table):
    m = x.shape[0]
    out = dot(jnp.concatenate(thirds(x), 0), table)
    return out[:m] + (out[m : 2 * m] + out[2 * m :])


def lanes_of(shape):
    return lax.broadcasted_iota(jnp.int32, shape, len(shape) - 1)


def rank_body(s1, s2, tiles, packed, slot1, slot2, table, lhs, rhs, stage):
    col = lax.axis_index("col")
    upper = (
        lax.broadcasted_iota(jnp.int32, (128, 128), 0) < lax.broadcasted_iota(jnp.int32, (128, 128), 1)
    ).astype(BF16)
    groups = lax.broadcasted_iota(jnp.int32, (16, 128), 0)
    ranks = []
    for which, (source, target) in enumerate(((s1, slot1), (s2, slot2))):
        carry = jnp.zeros((16, 1), F32)
        rank = []
        for m in range(12):
            row = source[m : m + 1, :]
            group = jnp.bitwise_and(lax.shift_right_logical(row, 5), 15)
            inside = row < 4608
            mark = ((group == groups) & inside).astype(F32)
            before = dot(mark.astype(BF16), upper) + carry
            t = jnp.sum(mark * before, axis=0, keepdims=True)
            carry = carry + jnp.sum(mark, axis=1, keepdims=True)
            rank.append(t + 1.0)
            place = group * SLOTS + t.astype(jnp.int32)
            if which:
                place = jnp.where(inside, place, EXT)
            target[m : m + 1, :] = place
        ranks.append(rank)
    slots = lanes_of((32, 128)).astype(F32)
    table[288:, :] = jnp.zeros((96, 256), BF16)
    for j in range(9):
        spots = lax.broadcasted_iota(jnp.int32, (32, 128), 0) + (j * 512 + col * 32)
        both = []
        for source, rank in ((s1, ranks[0]), (s2, ranks[1])):
            total = jnp.zeros((32, 128), F32)
            for m in range(12):
                total = total + jnp.where(source[m : m + 1, :] == spots, rank[m], 0.0)
            slot = jnp.sum(total, axis=1, keepdims=True) - 1.0
            both.append((slot == slots).astype(BF16))
        pair = jnp.concatenate(both, 1)
        table[j * 32 : (j + 1) * 32, :] = pair
        for al in range(4):
            rhs[j * 128 + al * 32 : j * 128 + (al + 1) * 32, :] = pair
        quarter = lanes_of((4, 128)) // 32
        for i in range(9):
            for al in range(4):
                stage[i * 16 + al * 4 : i * 16 + (al + 1) * 4, :] = jnp.where(quarter == al, tiles[i, j], 0.0)
        for part, value in enumerate(thirds(stage[...])):
            lhs[part * TALL : (part + 1) * TALL, j * 128 : (j + 1) * 128] = value
    out = dot(lhs[...], rhs[...])
    packed[...] = out[:TALL] + (out[TALL : 2 * TALL] + out[2 * TALL :])


def list_body(s2, later):
    upper = (
        lax.broadcasted_iota(jnp.int32, (128, 128), 0) < lax.broadcasted_iota(jnp.int32, (128, 128), 1)
    ).astype(BF16)
    row = s2[...]
    group = jnp.bitwise_and(lax.shift_right_logical(row, 5), 15)
    high = lax.shift_right_logical(row - 4608, 9)
    other = group * 64 + high * 32 + jnp.bitwise_and(row, 31)
    mark = jnp.where(row < 4608, 0.0, 1.0)
    order = dot(jnp.concatenate([mark, mark[:4]], 0).astype(BF16), upper)[:12]
    total = jnp.sum(mark, axis=1, keepdims=True)
    count = jnp.zeros((1, 1), F32)
    spot = lax.broadcasted_iota(jnp.int32, (384, 128), 0).astype(F32)
    kind = lax.broadcasted_iota(jnp.int32, (8, 128), 0)
    matches, values = [], []
    for m in range(12):
        place = jnp.where(mark[m : m + 1] > 0, order[m : m + 1] + count, -1.0)
        count = count + total[m : m + 1]
        index = lanes_of((1, 128)) + m * 128
        value = jnp.where(kind == 0, lax.shift_right_logical(index, 6), jnp.bitwise_and(index, 63))
        value = jnp.where(kind == 2, lax.shift_right_logical(other[m : m + 1], 6), value)
        value = jnp.where(kind == 3, jnp.bitwise_and(other[m : m + 1], 63), value)
        values.append(jnp.where(kind == 4, 1, value).astype(F32).astype(BF16))
        matches.append((place == spot).astype(BF16))
    listed = lax.dot_general(
        jnp.concatenate(values, 1),
        jnp.concatenate(matches, 1),
        (((1,), (1,)), ((), ())),
        preferred_element_type=F32,
    )
    source_row = listed[0:1] * 64.0 + listed[1:2]
    target_row = jnp.where(listed[4:5] > 0.5, listed[2:3] * 64.0 + listed[3:4], 1024.0)
    later[...] = jnp.concatenate([source_row, target_row], 0).astype(jnp.int32)


def lay_body(p1, p2, d1, panel, near, mixed, tall):
    tall[...] = jnp.zeros((128, 128), F32)
    tall[0:32, 0:48] = p1[0]
    tall[32:64, 0:48] = p1[1]
    tall[64:96, 0:48] = p2[0]
    both = tall[...].T[:48]
    lane = lanes_of((16, 128))
    value = jnp.zeros((16, 128), F32)
    for h in range(3):
        moved = pltpu.roll(both[16 * h : 16 * (h + 1)], (32 * h - 64) % 128, 1)
        value = jnp.where(lane // 32 == h, moved, value)
    for n in range(32):
        panel[n] = value
    near[...] = jnp.where(lanes_of((24, 128)) < 64, both[:24], pltpu.roll(both[24:], 64, 1))
    lane = lanes_of((4, 128))
    tall[0:48, :] = both
    for al in range(4):
        for k in range(2):
            value = jnp.zeros((4, 128), F32)
            for m in range(2):
                value = jnp.where(lane // 32 == m, pltpu.roll(d1[k, m], ((m - al) * 32) % 128, 1), value)
            tall[48 + al * 8 + k * 4 : 52 + al * 8 + k * 4, :] = value
    half = lanes_of((40, 128)) < 64
    value = jnp.where(half, tall[0:40, :], pltpu.roll(tall[40:80, :], 64, 1))
    for n in range(8):
        mixed[n] = value


def scatter_rows(slots, source, target):
    def place(step, _):
        base = pl.multiple_of(step * 48, 16)
        for u in range(48):
            target[pl.ds(slots[base + u], 1), :] = source[pl.ds(base + u, 1), :]
        return 0

    lax.fori_loop(0, 32, place, 0)


def in_order(step):
    return ((step % 8) * 4 + step // 8) * 48


def unfold(folds, rows):
    keep = lanes_of((16, 128))
    keep = (keep >= 64) & (keep < 96)
    for r in range(32):
        for h in range(3):
            moved = pltpu.roll(folds[r], (64 - 32 * h) % 128, 1)
            rows[r * 48 + 16 * h : r * 48 + 16 * (h + 1), :] = jnp.where(keep, moved, 0.0)


def second_body(later, panels, near, mine, other, spread, fold, extra, rows):
    unfold(panels, rows)
    spread[...] = jnp.zeros(spread.shape, F32)

    def place(step, _):
        for u in range(48):
            n = step * 48 + u
            spread[pl.ds(later[1, n], 1), :] = rows[pl.ds(later[0, n], 1), :]
        return 0

    lax.fori_loop(0, 8, place, 0)
    core = lax.axis_index("col") % 2
    half = lanes_of((40, 128)) < 64
    total = jnp.zeros((160, 256), F32)
    for z in range(8):
        left, right = [], []
        for source, k in ((mine, core), (other, 1 - core)):
            x = source[z]
            left.append(jnp.concatenate([jnp.where(half, x, 0.0), jnp.where(half, 0.0, x)], 0))
            right += 2 * [spread[pl.ds(pl.multiple_of((2 * z + k) * 64, 64), 64), :]]
        total = total + product_terms(jnp.concatenate(left, 1), jnp.concatenate(right, 0))
    out = folded(total)
    lane_f = lanes_of((16, 128))
    value = jnp.zeros((16, 128), F32)
    for h in range(3):
        moved = pltpu.roll(out[16 * h : 16 * (h + 1), :], (32 * h - 64) % 128, 1)
        value = jnp.where(lane_f // 32 == h, moved, value)
    value = jnp.concatenate([value, near[...]], 0)
    for n in range(8):
        fold[n] = value
    extra[...] = out[48:80, :]


def first_body(slot2, panels, spread, rows):
    unfold(panels, rows)
    spread[...] = jnp.zeros(spread.shape, F32)
    scatter_rows(slot2, rows, spread)


def image_body(slot1, folds, second_hbm, blocks, extra, choice, out, send0, send1, rows, held, second, right, done):
    send = (send0, send1)
    third = pltpu.make_async_copy(second_hbm.at[pl.ds(0, EXT)], second, done.at[0])
    arrival = pltpu.make_async_copy(blocks, held, done.at[1])
    leaving = pltpu.make_async_copy(right, out, done.at[2])
    third.start()
    arrival.start()
    lane = lanes_of((16, 128))
    for step in range(32):
        piece = folds[step // 8, step % 8]
        base = in_order(step)
        near = jnp.concatenate([piece[16:], pltpu.roll(piece[16:], 64, 1)], 0)
        for h in range(3):
            moved = jnp.where(lane < 96, -pltpu.roll(piece[:16], (64 - 32 * h) % 128, 1), 0.0)
            rows[base + 16 * h : base + 16 * (h + 1), :] = jnp.where(lane < 64, near[16 * h : 16 * (h + 1)], moved)
    right[...] = jnp.zeros(right.shape, F32)
    scatter_rows(slot1, rows, right)
    third.wait()
    right[...] = right[...] + pltpu.roll(second[...], 32, 1)
    leaving.start()
    arrival.wait()
    total = jnp.zeros((4 * TALL, 256), F32)
    for c in range(0, 16, 2):
        left = [jnp.concatenate([held[c, :, n : n + 128], held[c + 1, :, n : n + 128]], 1) for n in (0, 128)]
        total = total + product_terms(jnp.concatenate(left, 0), right[c * SLOTS : (c + 2) * SLOTS, :])
    out_terms = folded(total)
    image = out_terms[:TALL]
    late = lanes_of((TALL, 128))
    image = jnp.where((late >= 64) & (late < 96), image + pltpu.roll(out_terms[TALL:], 96, 1), image)
    image = jnp.concatenate([image, extra[...]], 0)
    sent = jnp.zeros((96, TALL + 32), F32)
    for part in thirds(image):
        sent = sent + lax.dot_general(choice[...], part, (((1,), (1,)), ((), ())), preferred_element_type=F32)
    lane = lanes_of((16, 128))
    pieces = []
    for h in range(2):
        rest = jnp.concatenate([sent[h * 48 : (h + 1) * 48, 128:], jnp.zeros((48, 80), F32)], 1)
        tail = jnp.where(lane < 16, rest[0:16], pltpu.roll(rest[16:32], 16, 1))
        tail = jnp.where(lane < 32, tail, pltpu.roll(rest[32:48], 32, 1))
        pieces.append(jnp.concatenate([sent[h * 48 : (h + 1) * 48, :128], tail], 0))
    parity = lax.axis_index("row") % 2
    for h in range(2):

        @pl.when(parity == h)
        def _(h=h):
            send[0][...] = pieces[h]
            send[1][...] = pieces[1 - h]

    leaving.wait()


def cross_body(got0, got1, order, table, whole, share, own):
    parity = lax.axis_index("row") % 2
    a, b = got0[...], got1[...]
    even = jnp.where(parity == 0, a, b)
    odd = jnp.where(parity == 0, b, a)
    parts = []
    for got in (even, odd):
        tail = got[48:64]
        parts.append(got[:48])
        parts.append(jnp.concatenate([tail, pltpu.roll(tail, 112, 1), pltpu.roll(tail, 96, 1)], 0))
    y = chosen(jnp.concatenate(parts, 1), order[...])
    close = chosen(y[:, :384], table[...])
    e = y[32:48, 384:512]
    own[...] = e
    lane = lanes_of((8, 128))
    e = jnp.where(lane < 64, e[:8], pltpu.roll(e[8:], 64, 1))
    e = jnp.concatenate([close[:, :128], close[32:48, 128:], e], 0)
    for n in range(8):
        share[n] = e
    whole[...] = y[:, :384]


def pack_body(whole, first, second):
    y = whole[...]
    lane = lanes_of((8, 128))
    lane2 = lanes_of((4, 128))
    for i in range(9):
        chunk = (i // 4) * 128
        one = jnp.zeros((8, 128), F32)
        two = jnp.zeros((4, 128), F32)
        for al in range(4):
            shift = ((al - i % 4) * 32) % 128
            moved = pltpu.roll(y[al * 8 : (al + 1) * 8, chunk : chunk + 128], shift, 1) if shift else y[al * 8 : (al + 1) * 8, chunk : chunk + 128]
            one = jnp.where(lane // 32 == al, moved, one)
            low = y[32 + al * 4 : 36 + al * 4, chunk : chunk + 128]
            moved = pltpu.roll(low, shift, 1) if shift else low
            two = jnp.where(lane2 // 32 == al, moved, two)
        first[0, i] = -one[0:4]
        first[1, i] = -one[4:8]
        second[0, i] = -two


def diagonal_body(mine, other, right, later, own, d1, d2, left1, left2, first, second):
    first[:, 0:9] = left1[...]
    second[:, 0:9] = left2[...]
    core = lax.axis_index("col") % 2
    lane_e = lanes_of((8, 128))
    total = jnp.zeros((128, 256), F32)
    also = jnp.zeros((32, 256), F32)
    for z in range(8):
        left, wide, extra, late = [], [], [], []
        for source, k in ((mine, core), (other, 1 - core)):
            c = 2 * z + k
            x = source[z]
            left.append(x[:64])
            wide.append(right[pl.ds(pl.multiple_of(c * SLOTS, SLOTS), SLOTS), :])
            e = x[64:72]
            extra.append(jnp.concatenate([jnp.where(lane_e < 64, e, 0.0), jnp.where(lane_e >= 64, e, 0.0)], 0))
            late += 2 * [later[pl.ds(pl.multiple_of(c * 64, 64), 64), :]]
        total = total + product_terms(jnp.concatenate(left, 1), jnp.concatenate(wide, 0))
        also = also + product_terms(jnp.concatenate(extra, 1), jnp.concatenate(late, 0))
    out = folded(total)
    g1 = out[:32]
    bottom = own[...] - out[32:48]
    g2 = out[32:48] + pltpu.roll(out[48:64], 96, 1) + folded(also)
    lane = lanes_of((8, 128))
    lane2 = lanes_of((4, 128))
    for k in range(2):
        one = jnp.zeros((8, 128), F32)
        two = jnp.zeros((4, 128), F32)
        for al in range(4):
            shift = ((al - k) * 32) % 128
            one = jnp.where(lane // 32 == al, pltpu.roll(g1[al * 8 : (al + 1) * 8], shift, 1), one)
            two = jnp.where(lane2 // 32 == al, pltpu.roll(bottom[al * 4 : (al + 1) * 4], shift, 1), two)
        first[0, 9 + k] = d1[0, k] + one[0:4]
        first[1, 9 + k] = d1[1, k] + one[4:8]
        second[0, 9 + k] = -two
    two = jnp.zeros((4, 128), F32)
    for al in range(4):
        shift = ((al - 2) * 32) % 128
        two = jnp.where(lane2 // 32 == al, pltpu.roll(g2[al * 4 : (al + 1) * 4], shift, 1), two)
    second[0, 11] = d2[0, 0] + two


VMEM = pl.BlockSpec(memory_space=pltpu.VMEM)
SMEM = pl.BlockSpec(memory_space=pltpu.SMEM)
ANY = pl.BlockSpec(memory_space=pl.ANY)


def kernel(body, specs, outs, scratch=(), places=None):
    return pl.pallas_call(
        body,
        in_specs=list(specs),
        out_specs=list(places or [VMEM] * len(outs)),
        out_shape=[jax.ShapeDtypeStruct(shape, dtype) for shape, dtype in outs],
        scratch_shapes=list(scratch),
    )


def exchanged(x, axis, groups):
    return lax.all_to_all(x, axis, 0, 0, axis_index_groups=groups, tiled=True)


def swapped(x):
    return lax.ppermute(x, "col", [(c, c ^ 1) for c in range(16)])


def transposed(x, turn):
    pairs = [(r * 16 + c, (2 * c + (r + turn) % 2) * 16 + r // 2) for r in range(32) for c in range(16)]
    return lax.ppermute(x, ("row", "col"), pairs)


def on_device(ancestor, inverse_first, panel_first, structure_first, inverse_second, panel_second, structure_second):
    panel, near, mixed = kernel(
        lay_body,
        (VMEM, VMEM, VMEM),
        (((32, 16, 128), F32), ((24, 128), F32), ((8, 40, 128), F32)),
        (pltpu.VMEM((128, 128), F32),),
    )(panel_first.transpose(1, 2, 0), panel_second.transpose(1, 2, 0), inverse_first)
    packed, slot1, slot2, table = kernel(
        rank_body,
        (VMEM, VMEM, VMEM),
        (
            ((TALL, 256), F32),
            ((12, 128), jnp.int32),
            ((12, 128), jnp.int32),
            ((384, 256), BF16),
        ),
        (pltpu.VMEM((3 * TALL, 1152), BF16), pltpu.VMEM((1152, 256), BF16), pltpu.VMEM((TALL, 128), F32)),
    )(structure_first.reshape(12, 128), structure_second.reshape(12, 128), ancestor)
    blocks = lax.all_gather(packed, "col")
    mine = exchanged(mixed, "col", Z_GROUPS)
    other = swapped(mine)
    panels = lax.all_to_all(panel, "row", 0, 0, tiled=True)
    (later,) = kernel(list_body, (VMEM,), (((2, 384), jnp.int32),))(structure_second.reshape(12, 128))
    slot1, slot2 = slot1.reshape(1536), slot2.reshape(1536)
    rows = pltpu.VMEM((1536, 128), F32)
    second, fold, extra = kernel(
        second_body,
        (SMEM, VMEM, VMEM, VMEM, VMEM),
        (((1032, 128), F32), ((8, 40, 128), F32), ((32, 128), F32)),
        (rows,),
    )(later, panels, near, mine, other)
    folds = exchanged(fold, "row", Y_GROUPS)
    folds = exchanged(jnp.broadcast_to(folds, (4, *folds.shape)), "row", X_GROUPS)
    (spread,) = kernel(first_body, (SMEM, VMEM), (((EXT + 8, 128), F32),), (rows,))(slot2, panels)
    big = pltpu.VMEM((EXT, 128), F32)
    right, send0, send1 = kernel(
        image_body,
        (SMEM, VMEM, ANY, ANY, VMEM, VMEM),
        (((EXT, 128), F32), ((64, 128), F32), ((64, 128), F32)),
        (rows, pltpu.VMEM((16, TALL, 256), F32), big, big, pltpu.SemaphoreType.DMA((3,))),
        (ANY, VMEM, VMEM),
    )(slot1, folds, spread, blocks, extra, jnp.asarray(column_choice(), BF16))
    got0, got1 = transposed(send0, 0), transposed(send1, 1)
    whole, share, own = kernel(
        cross_body,
        (VMEM, VMEM, VMEM, VMEM),
        (((48, 384), F32), ((8, 72, 128), F32), ((16, 128), F32)),
    )(got0, got1, jnp.asarray(lane_order(), BF16), table)
    mine = exchanged(share, "col", Z_GROUPS)
    left1, left2 = kernel(pack_body, (VMEM,), (((2, 9, 4, 128), F32), ((1, 9, 4, 128), F32)))(whole)
    other = swapped(mine)
    return kernel(
        diagonal_body,
        (VMEM,) * 9,
        (((2, 11, 4, 128), F32), ((1, 12, 4, 128), F32)),
    )(mine, other, right, second, own, inverse_first, inverse_second, left1, left2)


def solution(mesh):
    tiles = P(None, None, "row", "col")
    panels = P("row", None, "col")

    return jax.shard_map(
        on_device,
        mesh=mesh,
        in_specs=(tiles, tiles, panels, P(), tiles, panels, P()),
        out_specs=(tiles, tiles),
        check_vma=False,
    )
```

```python
import jax
import jax.numpy as jnp
import numpy as np
from jax import lax
from jax.experimental import pallas as pl
from jax.experimental.pallas import tpu as pltpu
from jax.sharding import PartitionSpec as P


F32 = jnp.float32
BF16 = jnp.bfloat16
TALL = 144
SLOTS = 128
EXT = 16 * SLOTS

Y_GROUPS = [[4 * y + x for y in range(8)] for x in range(4)]
X_GROUPS = [[4 * y + x for x in range(4)] for y in range(8)]
Z_GROUPS = [[2 * z + k for z in range(8)] for k in range(2)]


def column_choice():
    table = np.zeros((96, 128), np.float32)
    for h in range(2):
        for m in range(32):
            al, k, q = m // 8, (m % 8) // 4, m % 4
            table[h * 48 + m, k * 32 + h * 16 + 4 * q + al] = 1
        for m in range(16):
            al, q = m // 4, m % 4
            table[h * 48 + 32 + m, 64 + h * 16 + 4 * q + al] = 1
    return table


def lane_order():
    table = np.zeros((512, 512), np.float32)
    for g in range(2):
        for al in range(4):
            for i in range(9):
                for q in range(4):
                    table[g * 256 + i * 16 + al * 4 + q, i * 32 + g * 16 + 4 * q + al] = 1
            for k in range(2):
                for q in range(4):
                    table[g * 256 + TALL + al * 8 + k * 4 + q, 384 + k * 32 + g * 16 + 4 * q + al] = 1
    return table


def dot(left, right):
    return jnp.dot(left, right, preferred_element_type=F32)


def halves(x):
    high = x.astype(BF16)
    return high, (x - high.astype(F32)).astype(BF16)


def thirds(x):
    high = x.astype(BF16)
    rest = x - high.astype(F32)
    mid = rest.astype(BF16)
    return high, mid, (rest - mid.astype(F32)).astype(BF16)


def product_terms(left, right):
    return dot(jnp.concatenate(halves(left), 0), jnp.concatenate(halves(right), 1))


def folded(terms):
    m, n = terms.shape[0] // 2, terms.shape[1] // 2
    return terms[:m, :n] + (terms[:m, n:] + terms[m:, :n])


def chosen(x, table):
    m = x.shape[0]
    out = dot(jnp.concatenate(thirds(x), 0), table)
    return out[:m] + (out[m : 2 * m] + out[2 * m :])


def lanes_of(shape):
    return lax.broadcasted_iota(jnp.int32, shape, len(shape) - 1)


def rank_body(s1, s2, tiles, packed, slot1, slot2, table, lhs, rhs, stage):
    col = lax.axis_index("col")
    upper = (
        lax.broadcasted_iota(jnp.int32, (128, 128), 0) < lax.broadcasted_iota(jnp.int32, (128, 128), 1)
    ).astype(BF16)
    groups = lax.broadcasted_iota(jnp.int32, (16, 128), 0)
    ranks = []
    for which, (source, target) in enumerate(((s1, slot1), (s2, slot2))):
        carry = jnp.zeros((16, 1), F32)
        rank = []
        for m in range(12):
            row = source[m : m + 1, :]
            group = jnp.bitwise_and(lax.shift_right_logical(row, 5), 15)
            inside = row < 4608
            mark = ((group == groups) & inside).astype(F32)
            before = dot(mark.astype(BF16), upper) + carry
            t = jnp.sum(mark * before, axis=0, keepdims=True)
            carry = carry + jnp.sum(mark, axis=1, keepdims=True)
            rank.append(t + 1.0)
            place = group * SLOTS + t.astype(jnp.int32)
            if which:
                place = jnp.where(inside, place, EXT)
            target[m : m + 1, :] = place
        ranks.append(rank)
    slots = lanes_of((32, 128)).astype(F32)
    table[288:, :] = jnp.zeros((96, 256), BF16)
    for j in range(9):
        spots = lax.broadcasted_iota(jnp.int32, (32, 128), 0) + (j * 512 + col * 32)
        both = []
        for source, rank in ((s1, ranks[0]), (s2, ranks[1])):
            total = jnp.zeros((32, 128), F32)
            for m in range(12):
                total = total + jnp.where(source[m : m + 1, :] == spots, rank[m], 0.0)
            slot = jnp.sum(total, axis=1, keepdims=True) - 1.0
            both.append((slot == slots).astype(BF16))
        pair = jnp.concatenate(both, 1)
        table[j * 32 : (j + 1) * 32, :] = pair
        for al in range(4):
            rhs[j * 128 + al * 32 : j * 128 + (al + 1) * 32, :] = pair
        quarter = lanes_of((4, 128)) // 32
        for i in range(9):
            for al in range(4):
                stage[i * 16 + al * 4 : i * 16 + (al + 1) * 4, :] = jnp.where(quarter == al, tiles[i, j], 0.0)
        for part, value in enumerate(thirds(stage[...])):
            lhs[part * TALL : (part + 1) * TALL, j * 128 : (j + 1) * 128] = value
    out = dot(lhs[...], rhs[...])
    packed[...] = out[:TALL] + (out[TALL : 2 * TALL] + out[2 * TALL :])


def list_body(s2, later):
    upper = (
        lax.broadcasted_iota(jnp.int32, (128, 128), 0) < lax.broadcasted_iota(jnp.int32, (128, 128), 1)
    ).astype(BF16)
    row = s2[...]
    group = jnp.bitwise_and(lax.shift_right_logical(row, 5), 15)
    high = lax.shift_right_logical(row - 4608, 9)
    other = group * 64 + high * 32 + jnp.bitwise_and(row, 31)
    mark = jnp.where(row < 4608, 0.0, 1.0)
    order = dot(jnp.concatenate([mark, mark[:4]], 0).astype(BF16), upper)[:12]
    total = jnp.sum(mark, axis=1, keepdims=True)
    count = jnp.zeros((1, 1), F32)
    spot = lax.broadcasted_iota(jnp.int32, (384, 128), 0).astype(F32)
    kind = lax.broadcasted_iota(jnp.int32, (8, 128), 0)
    matches, values = [], []
    for m in range(12):
        place = jnp.where(mark[m : m + 1] > 0, order[m : m + 1] + count, -1.0)
        count = count + total[m : m + 1]
        index = lanes_of((1, 128)) + m * 128
        value = jnp.where(kind == 0, lax.shift_right_logical(index, 6), jnp.bitwise_and(index, 63))
        value = jnp.where(kind == 2, lax.shift_right_logical(other[m : m + 1], 6), value)
        value = jnp.where(kind == 3, jnp.bitwise_and(other[m : m + 1], 63), value)
        values.append(jnp.where(kind == 4, 1, value).astype(F32).astype(BF16))
        matches.append((place == spot).astype(BF16))
    listed = lax.dot_general(
        jnp.concatenate(values, 1),
        jnp.concatenate(matches, 1),
        (((1,), (1,)), ((), ())),
        preferred_element_type=F32,
    )
    source_row = listed[0:1] * 64.0 + listed[1:2]
    target_row = jnp.where(listed[4:5] > 0.5, listed[2:3] * 64.0 + listed[3:4], 1024.0)
    later[...] = jnp.concatenate([source_row, target_row], 0).astype(jnp.int32)


def lay_body(p1, p2, d1, panel, near, mixed, tall):
    tall[...] = jnp.zeros((128, 128), F32)
    tall[0:32, 0:48] = p1[0]
    tall[32:64, 0:48] = p1[1]
    tall[64:96, 0:48] = p2[0]
    both = tall[...].T[:48]
    lane = lanes_of((16, 128))
    value = jnp.zeros((16, 128), F32)
    for h in range(3):
        moved = pltpu.roll(both[16 * h : 16 * (h + 1)], (32 * h - 64) % 128, 1)
        value = jnp.where(lane // 32 == h, moved, value)
    for n in range(32):
        panel[n] = value
    near[...] = jnp.where(lanes_of((24, 128)) < 64, both[:24], pltpu.roll(both[24:], 64, 1))
    lane = lanes_of((4, 128))
    tall[0:48, :] = both
    for al in range(4):
        for k in range(2):
            value = jnp.zeros((4, 128), F32)
            for m in range(2):
                value = jnp.where(lane // 32 == m, pltpu.roll(d1[k, m], ((m - al) * 32) % 128, 1), value)
            tall[48 + al * 8 + k * 4 : 52 + al * 8 + k * 4, :] = value
    half = lanes_of((40, 128)) < 64
    value = jnp.where(half, tall[0:40, :], pltpu.roll(tall[40:80, :], 64, 1))
    for n in range(8):
        mixed[n] = value


def scatter_rows(slots, source, target):
    def place(step, _):
        base = pl.multiple_of(step * 48, 16)
        for u in range(48):
            target[pl.ds(slots[base + u], 1), :] = source[pl.ds(base + u, 1), :]
        return 0

    lax.fori_loop(0, 32, place, 0)


def in_order(step):
    return ((step % 8) * 4 + step // 8) * 48


def unfold(folds, rows):
    keep = lanes_of((16, 128))
    keep = (keep >= 64) & (keep < 96)
    for r in range(32):
        for h in range(3):
            moved = pltpu.roll(folds[r], (64 - 32 * h) % 128, 1)
            rows[r * 48 + 16 * h : r * 48 + 16 * (h + 1), :] = jnp.where(keep, moved, 0.0)


def second_body(later, panels, near, mine, other, spread, fold, extra, rows):
    unfold(panels, rows)
    spread[...] = jnp.zeros(spread.shape, F32)

    def place(step, _):
        for u in range(48):
            n = step * 48 + u
            spread[pl.ds(later[1, n], 1), :] = rows[pl.ds(later[0, n], 1), :]
        return 0

    lax.fori_loop(0, 8, place, 0)
    core = lax.axis_index("col") % 2
    half = lanes_of((40, 128)) < 64
    total = jnp.zeros((160, 256), F32)
    for z in range(8):
        left, right = [], []
        for source, k in ((mine, core), (other, 1 - core)):
            x = source[z]
            left.append(jnp.concatenate([jnp.where(half, x, 0.0), jnp.where(half, 0.0, x)], 0))
            right += 2 * [spread[pl.ds(pl.multiple_of((2 * z + k) * 64, 64), 64), :]]
        total = total + product_terms(jnp.concatenate(left, 1), jnp.concatenate(right, 0))
    out = folded(total)
    lane_f = lanes_of((16, 128))
    value = jnp.zeros((16, 128), F32)
    for h in range(3):
        moved = pltpu.roll(out[16 * h : 16 * (h + 1), :], (32 * h - 64) % 128, 1)
        value = jnp.where(lane_f // 32 == h, moved, value)
    value = jnp.concatenate([value, near[...]], 0)
    for n in range(8):
        fold[n] = value
    extra[...] = out[48:80, :]


def first_body(slot2, panels, spread, rows):
    unfold(panels, rows)
    spread[...] = jnp.zeros(spread.shape, F32)
    scatter_rows(slot2, rows, spread)


def image_body(slot1, folds, second_hbm, blocks, extra, choice, out, send, rows, held, second, right, done):
    third = pltpu.make_async_copy(second_hbm.at[pl.ds(0, EXT)], second, done.at[0])
    arrival = pltpu.make_async_copy(blocks, held, done.at[1])
    leaving = pltpu.make_async_copy(right, out, done.at[2])
    third.start()
    arrival.start()
    lane = lanes_of((16, 128))
    for step in range(32):
        piece = folds[step // 8, step % 8]
        base = in_order(step)
        near = jnp.concatenate([piece[16:], pltpu.roll(piece[16:], 64, 1)], 0)
        for h in range(3):
            moved = jnp.where(lane < 96, -pltpu.roll(piece[:16], (64 - 32 * h) % 128, 1), 0.0)
            rows[base + 16 * h : base + 16 * (h + 1), :] = jnp.where(lane < 64, near[16 * h : 16 * (h + 1)], moved)
    right[...] = jnp.zeros(right.shape, F32)
    scatter_rows(slot1, rows, right)
    third.wait()
    right[...] = right[...] + pltpu.roll(second[...], 32, 1)
    leaving.start()
    arrival.wait()
    total = jnp.zeros((4 * TALL, 256), F32)
    for c in range(0, 16, 2):
        left = [jnp.concatenate([held[c, :, n : n + 128], held[c + 1, :, n : n + 128]], 1) for n in (0, 128)]
        total = total + product_terms(jnp.concatenate(left, 0), right[c * SLOTS : (c + 2) * SLOTS, :])
    out_terms = folded(total)
    image = out_terms[:TALL]
    late = lanes_of((TALL, 128))
    image = jnp.where((late >= 64) & (late < 96), image + pltpu.roll(out_terms[TALL:], 96, 1), image)
    image = jnp.concatenate([image, extra[...]], 0)
    sent = jnp.zeros((96, TALL + 32), F32)
    for part in thirds(image):
        sent = sent + lax.dot_general(choice[...], part, (((1,), (1,)), ((), ())), preferred_element_type=F32)
    lane = lanes_of((16, 128))
    pieces = []
    for h in range(2):
        rest = jnp.concatenate([sent[h * 48 : (h + 1) * 48, 128:], jnp.zeros((48, 80), F32)], 1)
        tail = jnp.where(lane < 16, rest[0:16], pltpu.roll(rest[16:32], 16, 1))
        tail = jnp.where(lane < 32, tail, pltpu.roll(rest[32:48], 32, 1))
        pieces.append(jnp.concatenate([sent[h * 48 : (h + 1) * 48, :128], tail], 0))
    place = mirror_place()
    send[...] = jnp.zeros(send.shape, F32)
    for h in range(2):
        send[pl.ds(place + h, 1)] = pieces[h][None]
    leaving.wait()


def cross_body(got, order, table, whole, share, own):
    place = mirror_place()
    parts = []
    for g in range(2):
        piece = got[pl.ds(place + g, 1)][0]
        tail = piece[48:64]
        parts.append(piece[:48])
        parts.append(jnp.concatenate([tail, pltpu.roll(tail, 112, 1), pltpu.roll(tail, 96, 1)], 0))
    y = chosen(jnp.concatenate(parts, 1), order[...])
    close = chosen(y[:, :384], table[...])
    e = y[32:48, 384:512]
    own[...] = e
    lane = lanes_of((8, 128))
    e = jnp.where(lane < 64, e[:8], pltpu.roll(e[8:], 64, 1))
    e = jnp.concatenate([close[:, :128], close[32:48, 128:], e], 0)
    for n in range(8):
        share[n] = e
    whole[...] = y[:, :384]


def pack_body(whole, first, second):
    y = whole[...]
    lane = lanes_of((8, 128))
    lane2 = lanes_of((4, 128))
    for i in range(9):
        chunk = (i // 4) * 128
        one = jnp.zeros((8, 128), F32)
        two = jnp.zeros((4, 128), F32)
        for al in range(4):
            shift = ((al - i % 4) * 32) % 128
            moved = pltpu.roll(y[al * 8 : (al + 1) * 8, chunk : chunk + 128], shift, 1) if shift else y[al * 8 : (al + 1) * 8, chunk : chunk + 128]
            one = jnp.where(lane // 32 == al, moved, one)
            low = y[32 + al * 4 : 36 + al * 4, chunk : chunk + 128]
            moved = pltpu.roll(low, shift, 1) if shift else low
            two = jnp.where(lane2 // 32 == al, moved, two)
        first[0, i] = -one[0:4]
        first[1, i] = -one[4:8]
        second[0, i] = -two


def diagonal_body(mine, other, right, later, own, d1, d2, left1, left2, first, second):
    first[:, 0:9] = left1[...]
    second[:, 0:9] = left2[...]
    core = lax.axis_index("col") % 2
    lane_e = lanes_of((8, 128))
    total = jnp.zeros((128, 256), F32)
    also = jnp.zeros((32, 256), F32)
    for z in range(8):
        left, wide, extra, late = [], [], [], []
        for source, k in ((mine, core), (other, 1 - core)):
            c = 2 * z + k
            x = source[z]
            left.append(x[:64])
            wide.append(right[pl.ds(pl.multiple_of(c * SLOTS, SLOTS), SLOTS), :])
            e = x[64:72]
            extra.append(jnp.concatenate([jnp.where(lane_e < 64, e, 0.0), jnp.where(lane_e >= 64, e, 0.0)], 0))
            late += 2 * [later[pl.ds(pl.multiple_of(c * 64, 64), 64), :]]
        total = total + product_terms(jnp.concatenate(left, 1), jnp.concatenate(wide, 0))
        also = also + product_terms(jnp.concatenate(extra, 1), jnp.concatenate(late, 0))
    out = folded(total)
    g1 = out[:32]
    bottom = own[...] - out[32:48]
    g2 = out[32:48] + pltpu.roll(out[48:64], 96, 1) + folded(also)
    lane = lanes_of((8, 128))
    lane2 = lanes_of((4, 128))
    for k in range(2):
        one = jnp.zeros((8, 128), F32)
        two = jnp.zeros((4, 128), F32)
        for al in range(4):
            shift = ((al - k) * 32) % 128
            one = jnp.where(lane // 32 == al, pltpu.roll(g1[al * 8 : (al + 1) * 8], shift, 1), one)
            two = jnp.where(lane2 // 32 == al, pltpu.roll(bottom[al * 4 : (al + 1) * 4], shift, 1), two)
        first[0, 9 + k] = d1[0, k] + one[0:4]
        first[1, 9 + k] = d1[1, k] + one[4:8]
        second[0, 9 + k] = -two
    two = jnp.zeros((4, 128), F32)
    for al in range(4):
        shift = ((al - 2) * 32) % 128
        two = jnp.where(lane2 // 32 == al, pltpu.roll(g2[al * 4 : (al + 1) * 4], shift, 1), two)
    second[0, 11] = d2[0, 0] + two


VMEM = pl.BlockSpec(memory_space=pltpu.VMEM)
SMEM = pl.BlockSpec(memory_space=pltpu.SMEM)
ANY = pl.BlockSpec(memory_space=pl.ANY)


def kernel(body, specs, outs, scratch=(), places=None):
    return pl.pallas_call(
        body,
        in_specs=list(specs),
        out_specs=list(places or [VMEM] * len(outs)),
        out_shape=[jax.ShapeDtypeStruct(shape, dtype) for shape, dtype in outs],
        scratch_shapes=list(scratch),
    )


def exchanged(x, axis, groups):
    return lax.all_to_all(x, axis, 0, 0, axis_index_groups=groups, tiled=True)


def swapped(x):
    return lax.ppermute(x, "col", [(c, c ^ 1) for c in range(16)])


def mirror_groups():
    def pair(u, v):
        return [(2 * u) * 16 + v, (2 * u + 1) * 16 + v]

    groups = [pair(u, v) + pair(v, u) for u in range(16) for v in range(u + 1, 16)]
    return groups + [pair(u, u) + pair(u + 1, u + 1) for u in range(0, 16, 2)]


def mirror_place():
    u, v = lax.axis_index("row") // 2, lax.axis_index("col")
    return jnp.where(u == v, (u % 2) * 2, jnp.where(u < v, 2, 0))


def on_device(ancestor, inverse_first, panel_first, structure_first, inverse_second, panel_second, structure_second):
    panel, near, mixed = kernel(
        lay_body,
        (VMEM, VMEM, VMEM),
        (((32, 16, 128), F32), ((24, 128), F32), ((8, 40, 128), F32)),
        (pltpu.VMEM((128, 128), F32),),
    )(panel_first.transpose(1, 2, 0), panel_second.transpose(1, 2, 0), inverse_first)
    packed, slot1, slot2, table = kernel(
        rank_body,
        (VMEM, VMEM, VMEM),
        (
            ((TALL, 256), F32),
            ((12, 128), jnp.int32),
            ((12, 128), jnp.int32),
            ((384, 256), BF16),
        ),
        (pltpu.VMEM((3 * TALL, 1152), BF16), pltpu.VMEM((1152, 256), BF16), pltpu.VMEM((TALL, 128), F32)),
    )(structure_first.reshape(12, 128), structure_second.reshape(12, 128), ancestor)
    blocks = lax.all_gather(packed, "col")
    mine = exchanged(mixed, "col", Z_GROUPS)
    other = swapped(mine)
    panels = lax.all_to_all(panel, "row", 0, 0, tiled=True)
    (later,) = kernel(list_body, (VMEM,), (((2, 384), jnp.int32),))(structure_second.reshape(12, 128))
    slot1, slot2 = slot1.reshape(1536), slot2.reshape(1536)
    rows = pltpu.VMEM((1536, 128), F32)
    second, fold, extra = kernel(
        second_body,
        (SMEM, VMEM, VMEM, VMEM, VMEM),
        (((1032, 128), F32), ((8, 40, 128), F32), ((32, 128), F32)),
        (rows,),
    )(later, panels, near, mine, other)
    folds = exchanged(fold, "row", Y_GROUPS)
    folds = exchanged(jnp.broadcast_to(folds, (4, *folds.shape)), "row", X_GROUPS)
    (spread,) = kernel(first_body, (SMEM, VMEM), (((EXT + 8, 128), F32),), (rows,))(slot2, panels)
    big = pltpu.VMEM((EXT, 128), F32)
    right, send = kernel(
        image_body,
        (SMEM, VMEM, ANY, ANY, VMEM, VMEM),
        (((EXT, 128), F32), ((4, 64, 128), F32)),
        (rows, pltpu.VMEM((16, TALL, 256), F32), big, big, pltpu.SemaphoreType.DMA((3,))),
        (ANY, VMEM),
    )(slot1, folds, spread, blocks, extra, jnp.asarray(column_choice(), BF16))
    got = exchanged(send, ("row", "col"), mirror_groups())
    whole, share, own = kernel(
        cross_body,
        (VMEM, VMEM, VMEM),
        (((48, 384), F32), ((8, 72, 128), F32), ((16, 128), F32)),
    )(got, jnp.asarray(lane_order(), BF16), table)
    mine = exchanged(share, "col", Z_GROUPS)
    left1, left2 = kernel(pack_body, (VMEM,), (((2, 9, 4, 128), F32), ((1, 9, 4, 128), F32)))(whole)
    other = swapped(mine)
    return kernel(
        diagonal_body,
        (VMEM,) * 9,
        (((2, 11, 4, 128), F32), ((1, 12, 4, 128), F32)),
    )(mine, other, right, second, own, inverse_first, inverse_second, left1, left2)


def solution(mesh):
    tiles = P(None, None, "row", "col")
    panels = P("row", None, "col")

    return jax.shard_map(
        on_device,
        mesh=mesh,
        in_specs=(tiles, tiles, panels, P(), tiles, panels, P()),
        out_specs=(tiles, tiles),
        check_vma=False,
    )
```

```python
import jax
import jax.numpy as jnp
import numpy as np
from jax import lax
from jax.experimental import pallas as pl
from jax.experimental.pallas import tpu as pltpu
from jax.sharding import PartitionSpec as P


F32 = jnp.float32
BF16 = jnp.bfloat16
TALL = 144
SLOTS = 128
EXT = 16 * SLOTS

Y_GROUPS = [[4 * y + x for y in range(8)] for x in range(4)]
X_GROUPS = [[4 * y + x for x in range(4)] for y in range(8)]
Z_GROUPS = [[2 * z + k for z in range(8)] for k in range(2)]


def column_choice():
    table = np.zeros((96, 128), np.float32)
    for h in range(2):
        for m in range(32):
            al, k, q = m // 8, (m % 8) // 4, m % 4
            table[h * 48 + m, k * 32 + h * 16 + 4 * q + al] = 1
        for m in range(16):
            al, q = m // 4, m % 4
            table[h * 48 + 32 + m, 64 + h * 16 + 4 * q + al] = 1
    return table


def lane_order():
    table = np.zeros((512, 512), np.float32)
    for g in range(2):
        for al in range(4):
            for i in range(9):
                for q in range(4):
                    table[g * 256 + i * 16 + al * 4 + q, i * 32 + g * 16 + 4 * q + al] = 1
            for k in range(2):
                for q in range(4):
                    table[g * 256 + TALL + al * 8 + k * 4 + q, 384 + k * 32 + g * 16 + 4 * q + al] = 1
    return table


def dot(left, right):
    return jnp.dot(left, right, preferred_element_type=F32)


def halves(x):
    high = x.astype(BF16)
    return high, (x - high.astype(F32)).astype(BF16)


def thirds(x):
    high = x.astype(BF16)
    rest = x - high.astype(F32)
    mid = rest.astype(BF16)
    return high, mid, (rest - mid.astype(F32)).astype(BF16)


def product_terms(left, right):
    return dot(jnp.concatenate(halves(left), 0), jnp.concatenate(halves(right), 1))


def folded(terms):
    m, n = terms.shape[0] // 2, terms.shape[1] // 2
    return terms[:m, :n] + (terms[:m, n:] + terms[m:, :n])


def chosen(x, table):
    m = x.shape[0]
    out = dot(jnp.concatenate(thirds(x), 0), table)
    return out[:m] + (out[m : 2 * m] + out[2 * m :])


def lanes_of(shape):
    return lax.broadcasted_iota(jnp.int32, shape, len(shape) - 1)


def rank_body(s1, s2, tiles, packed, slot1, slot2, table, lhs, rhs, stage):
    col = lax.axis_index("col")
    upper = (
        lax.broadcasted_iota(jnp.int32, (128, 128), 0) < lax.broadcasted_iota(jnp.int32, (128, 128), 1)
    ).astype(BF16)
    groups = lax.broadcasted_iota(jnp.int32, (16, 128), 0)
    ranks = []
    for which, (source, target) in enumerate(((s1, slot1), (s2, slot2))):
        carry = jnp.zeros((16, 1), F32)
        rank = []
        for m in range(12):
            row = source[m : m + 1, :]
            group = jnp.bitwise_and(lax.shift_right_logical(row, 5), 15)
            inside = row < 4608
            mark = ((group == groups) & inside).astype(F32)
            before = dot(mark.astype(BF16), upper) + carry
            t = jnp.sum(mark * before, axis=0, keepdims=True)
            carry = carry + jnp.sum(mark, axis=1, keepdims=True)
            rank.append(t + 1.0)
            place = group * SLOTS + t.astype(jnp.int32)
            if which:
                place = jnp.where(inside, place, EXT)
            target[m : m + 1, :] = place
        ranks.append(rank)
    slots = lanes_of((32, 128)).astype(F32)
    table[288:, :] = jnp.zeros((96, 256), BF16)
    for j in range(9):
        spots = lax.broadcasted_iota(jnp.int32, (32, 128), 0) + (j * 512 + col * 32)
        both = []
        for source, rank in ((s1, ranks[0]), (s2, ranks[1])):
            total = jnp.zeros((32, 128), F32)
            for m in range(12):
                total = total + jnp.where(source[m : m + 1, :] == spots, rank[m], 0.0)
            slot = jnp.sum(total, axis=1, keepdims=True) - 1.0
            both.append((slot == slots).astype(BF16))
        pair = jnp.concatenate(both, 1)
        table[j * 32 : (j + 1) * 32, :] = pair
        for al in range(4):
            rhs[j * 128 + al * 32 : j * 128 + (al + 1) * 32, :] = pair
        quarter = lanes_of((4, 128)) // 32
        for i in range(9):
            for al in range(4):
                stage[i * 16 + al * 4 : i * 16 + (al + 1) * 4, :] = jnp.where(quarter == al, tiles[i, j], 0.0)
        for part, value in enumerate(thirds(stage[...])):
            lhs[part * TALL : (part + 1) * TALL, j * 128 : (j + 1) * 128] = value
    out = dot(lhs[...], rhs[...])
    packed[...] = out[:TALL] + (out[TALL : 2 * TALL] + out[2 * TALL :])


def list_body(s2, later):
    upper = (
        lax.broadcasted_iota(jnp.int32, (128, 128), 0) < lax.broadcasted_iota(jnp.int32, (128, 128), 1)
    ).astype(BF16)
    row = s2[...]
    group = jnp.bitwise_and(lax.shift_right_logical(row, 5), 15)
    high = lax.shift_right_logical(row - 4608, 9)
    other = group * 64 + high * 32 + jnp.bitwise_and(row, 31)
    mark = jnp.where(row < 4608, 0.0, 1.0)
    order = dot(jnp.concatenate([mark, mark[:4]], 0).astype(BF16), upper)[:12]
    total = jnp.sum(mark, axis=1, keepdims=True)
    count = jnp.zeros((1, 1), F32)
    spot = lax.broadcasted_iota(jnp.int32, (384, 128), 0).astype(F32)
    kind = lax.broadcasted_iota(jnp.int32, (8, 128), 0)
    matches, values = [], []
    for m in range(12):
        place = jnp.where(mark[m : m + 1] > 0, order[m : m + 1] + count, -1.0)
        count = count + total[m : m + 1]
        index = lanes_of((1, 128)) + m * 128
        value = jnp.where(kind == 0, lax.shift_right_logical(index, 6), jnp.bitwise_and(index, 63))
        value = jnp.where(kind == 2, lax.shift_right_logical(other[m : m + 1], 6), value)
        value = jnp.where(kind == 3, jnp.bitwise_and(other[m : m + 1], 63), value)
        values.append(jnp.where(kind == 4, 1, value).astype(F32).astype(BF16))
        matches.append((place == spot).astype(BF16))
    listed = lax.dot_general(
        jnp.concatenate(values, 1),
        jnp.concatenate(matches, 1),
        (((1,), (1,)), ((), ())),
        preferred_element_type=F32,
    )
    source_row = listed[0:1] * 64.0 + listed[1:2]
    target_row = jnp.where(listed[4:5] > 0.5, listed[2:3] * 64.0 + listed[3:4], 1024.0)
    later[...] = jnp.concatenate([source_row, target_row], 0).astype(jnp.int32)


def lay_body(p1, p2, d1, panel, near, mixed, tall):
    tall[...] = jnp.zeros((128, 128), F32)
    tall[0:32, 0:48] = p1[0]
    tall[32:64, 0:48] = p1[1]
    tall[64:96, 0:48] = p2[0]
    both = tall[...].T[:48]
    lane = lanes_of((16, 128))
    value = jnp.zeros((16, 128), F32)
    for h in range(3):
        moved = pltpu.roll(both[16 * h : 16 * (h + 1)], (32 * h - 64) % 128, 1)
        value = jnp.where(lane // 32 == h, moved, value)
    for n in range(32):
        panel[n] = value
    near[...] = jnp.where(lanes_of((24, 128)) < 64, both[:24], pltpu.roll(both[24:], 64, 1))
    lane = lanes_of((4, 128))
    tall[0:48, :] = both
    for al in range(4):
        for k in range(2):
            value = jnp.zeros((4, 128), F32)
            for m in range(2):
                value = jnp.where(lane // 32 == m, pltpu.roll(d1[k, m], ((m - al) * 32) % 128, 1), value)
            tall[48 + al * 8 + k * 4 : 52 + al * 8 + k * 4, :] = value
    half = lanes_of((40, 128)) < 64
    value = jnp.where(half, tall[0:40, :], pltpu.roll(tall[40:80, :], 64, 1))
    for n in range(8):
        mixed[n] = value


def scatter_rows(slots, source, target):
    def place(step, _):
        base = pl.multiple_of(step * 48, 16)
        for u in range(48):
            target[pl.ds(slots[base + u], 1), :] = source[pl.ds(base + u, 1), :]
        return 0

    lax.fori_loop(0, 32, place, 0)


def in_order(step):
    return ((step % 8) * 4 + step // 8) * 48


def unfold(folds, rows, low):
    keep = lanes_of((16, 128))
    keep = (keep >= low) & (keep < low + 32)
    for r in range(32):
        for h in range(3):
            moved = pltpu.roll(folds[r], (low - 32 * h) % 128, 1)
            rows[r * 48 + 16 * h : r * 48 + 16 * (h + 1), :] = jnp.where(keep, moved, 0.0)


def second_body(later, panels, near, mine, other, spread, fold, extra, rows):
    unfold(panels, rows, 64)
    spread[...] = jnp.zeros(spread.shape, F32)

    def place(step, _):
        for u in range(48):
            n = step * 48 + u
            spread[pl.ds(later[1, n], 1), :] = rows[pl.ds(later[0, n], 1), :]
        return 0

    lax.fori_loop(0, 8, place, 0)
    core = lax.axis_index("col") % 2
    half = lanes_of((40, 128)) < 64
    total = jnp.zeros((160, 256), F32)
    for z in range(8):
        left, right = [], []
        for source, k in ((mine, core), (other, 1 - core)):
            x = source[z]
            left.append(jnp.concatenate([jnp.where(half, x, 0.0), jnp.where(half, 0.0, x)], 0))
            right += 2 * [spread[pl.ds(pl.multiple_of((2 * z + k) * 64, 64), 64), :]]
        total = total + product_terms(jnp.concatenate(left, 1), jnp.concatenate(right, 0))
    out = folded(total)
    lane_f = lanes_of((16, 128))
    value = jnp.zeros((16, 128), F32)
    for h in range(3):
        moved = pltpu.roll(out[16 * h : 16 * (h + 1), :], (32 * h - 64) % 128, 1)
        value = jnp.where(lane_f // 32 == h, moved, value)
    value = jnp.concatenate([value, near[...]], 0)
    for n in range(8):
        fold[n] = value
    extra[...] = out[48:80, :]


def first_body(slot2, panels, spread, rows):
    unfold(panels, rows, 96)
    spread[...] = jnp.zeros(spread.shape, F32)
    scatter_rows(slot2, rows, spread)


def image_body(slot1, folds, second_hbm, blocks, extra, choice, out, send, rows, held, second, right, done):
    third = pltpu.make_async_copy(second_hbm.at[pl.ds(0, EXT)], second, done.at[0])
    arrival = pltpu.make_async_copy(blocks, held, done.at[1])
    leaving = pltpu.make_async_copy(right, out, done.at[2])
    third.start()
    arrival.start()
    lane = lanes_of((16, 128))
    for step in range(32):
        piece = folds[step // 8, step % 8]
        base = in_order(step)
        near = jnp.concatenate([piece[16:], pltpu.roll(piece[16:], 64, 1)], 0)
        for h in range(3):
            moved = jnp.where(lane < 96, -pltpu.roll(piece[:16], (64 - 32 * h) % 128, 1), 0.0)
            rows[base + 16 * h : base + 16 * (h + 1), :] = jnp.where(lane < 64, near[16 * h : 16 * (h + 1)], moved)
    right[...] = jnp.zeros(right.shape, F32)
    scatter_rows(slot1, rows, right)
    third.wait()
    right[...] = right[...] + second[...]
    leaving.start()
    arrival.wait()
    total = jnp.zeros((4 * TALL, 256), F32)
    for c in range(0, 16, 2):
        left = [jnp.concatenate([held[c, :, n : n + 128], held[c + 1, :, n : n + 128]], 1) for n in (0, 128)]
        total = total + product_terms(jnp.concatenate(left, 0), right[c * SLOTS : (c + 2) * SLOTS, :])
    out_terms = folded(total)
    image = out_terms[:TALL]
    late = lanes_of((TALL, 128))
    image = jnp.where((late >= 64) & (late < 96), image + pltpu.roll(out_terms[TALL:], 96, 1), image)
    image = jnp.concatenate([image, extra[...]], 0)
    sent = jnp.zeros((96, TALL + 32), F32)
    for part in thirds(image):
        sent = sent + lax.dot_general(choice[...], part, (((1,), (1,)), ((), ())), preferred_element_type=F32)
    lane = lanes_of((16, 128))
    pieces = []
    for h in range(2):
        rest = jnp.concatenate([sent[h * 48 : (h + 1) * 48, 128:], jnp.zeros((48, 80), F32)], 1)
        tail = jnp.where(lane < 16, rest[0:16], pltpu.roll(rest[16:32], 16, 1))
        tail = jnp.where(lane < 32, tail, pltpu.roll(rest[32:48], 32, 1))
        pieces.append(jnp.concatenate([sent[h * 48 : (h + 1) * 48, :128], tail], 0))
    place = mirror_place()
    send[...] = jnp.zeros(send.shape, F32)
    for h in range(2):
        send[pl.ds(place + h, 1)] = pieces[h][None]
    leaving.wait()


def cross_body(got, order, table, whole, share, own):
    place = mirror_place()
    parts = []
    for g in range(2):
        piece = got[pl.ds(place + g, 1)][0]
        tail = piece[48:64]
        parts.append(piece[:48])
        parts.append(jnp.concatenate([tail, pltpu.roll(tail, 112, 1), pltpu.roll(tail, 96, 1)], 0))
    y = chosen(jnp.concatenate(parts, 1), order[...])
    close = chosen(y[:, :384], table[...])
    e = y[32:48, 384:512]
    own[...] = e
    lane = lanes_of((8, 128))
    e = jnp.where(lane < 64, e[:8], pltpu.roll(e[8:], 64, 1))
    e = jnp.concatenate([close[:, :128], close[32:48, 128:], e], 0)
    for n in range(8):
        share[n] = e
    whole[...] = y[:, :384]


def pack_body(whole, first, second):
    y = whole[...]
    lane = lanes_of((8, 128))
    lane2 = lanes_of((4, 128))
    for i in range(9):
        chunk = (i // 4) * 128
        one = jnp.zeros((8, 128), F32)
        two = jnp.zeros((4, 128), F32)
        for al in range(4):
            shift = ((al - i % 4) * 32) % 128
            moved = pltpu.roll(y[al * 8 : (al + 1) * 8, chunk : chunk + 128], shift, 1) if shift else y[al * 8 : (al + 1) * 8, chunk : chunk + 128]
            one = jnp.where(lane // 32 == al, moved, one)
            low = y[32 + al * 4 : 36 + al * 4, chunk : chunk + 128]
            moved = pltpu.roll(low, shift, 1) if shift else low
            two = jnp.where(lane2 // 32 == al, moved, two)
        first[0, i] = -one[0:4]
        first[1, i] = -one[4:8]
        second[0, i] = -two


def diagonal_body(mine, other, right, later, own, d1, d2, left1, left2, first, second):
    first[:, 0:9] = left1[...]
    second[:, 0:9] = left2[...]
    core = lax.axis_index("col") % 2
    lane_e = lanes_of((8, 128))
    total = jnp.zeros((128, 256), F32)
    also = jnp.zeros((32, 256), F32)
    for z in range(8):
        left, wide, extra, late = [], [], [], []
        for source, k in ((mine, core), (other, 1 - core)):
            c = 2 * z + k
            x = source[z]
            left.append(x[:64])
            wide.append(right[pl.ds(pl.multiple_of(c * SLOTS, SLOTS), SLOTS), :])
            e = x[64:72]
            extra.append(jnp.concatenate([jnp.where(lane_e < 64, e, 0.0), jnp.where(lane_e >= 64, e, 0.0)], 0))
            late += 2 * [later[pl.ds(pl.multiple_of(c * 64, 64), 64), :]]
        total = total + product_terms(jnp.concatenate(left, 1), jnp.concatenate(wide, 0))
        also = also + product_terms(jnp.concatenate(extra, 1), jnp.concatenate(late, 0))
    out = folded(total)
    g1 = out[:32]
    bottom = own[...] - out[32:48]
    g2 = out[32:48] + pltpu.roll(out[48:64], 96, 1) + folded(also)
    lane = lanes_of((8, 128))
    lane2 = lanes_of((4, 128))
    for k in range(2):
        one = jnp.zeros((8, 128), F32)
        two = jnp.zeros((4, 128), F32)
        for al in range(4):
            shift = ((al - k) * 32) % 128
            one = jnp.where(lane // 32 == al, pltpu.roll(g1[al * 8 : (al + 1) * 8], shift, 1), one)
            two = jnp.where(lane2 // 32 == al, pltpu.roll(bottom[al * 4 : (al + 1) * 4], shift, 1), two)
        first[0, 9 + k] = d1[0, k] + one[0:4]
        first[1, 9 + k] = d1[1, k] + one[4:8]
        second[0, 9 + k] = -two
    two = jnp.zeros((4, 128), F32)
    for al in range(4):
        shift = ((al - 2) * 32) % 128
        two = jnp.where(lane2 // 32 == al, pltpu.roll(g2[al * 4 : (al + 1) * 4], shift, 1), two)
    second[0, 11] = d2[0, 0] + two


VMEM = pl.BlockSpec(memory_space=pltpu.VMEM)
SMEM = pl.BlockSpec(memory_space=pltpu.SMEM)
ANY = pl.BlockSpec(memory_space=pl.ANY)


def kernel(body, specs, outs, scratch=(), places=None):
    return pl.pallas_call(
        body,
        in_specs=list(specs),
        out_specs=list(places or [VMEM] * len(outs)),
        out_shape=[jax.ShapeDtypeStruct(shape, dtype) for shape, dtype in outs],
        scratch_shapes=list(scratch),
    )


def exchanged(x, axis, groups):
    return lax.all_to_all(x, axis, 0, 0, axis_index_groups=groups, tiled=True)


def swapped(x):
    return lax.ppermute(x, "col", [(c, c ^ 1) for c in range(16)])


def mirror_groups():
    def pair(u, v):
        return [(2 * u) * 16 + v, (2 * u + 1) * 16 + v]

    groups = [pair(u, v) + pair(v, u) for u in range(16) for v in range(u + 1, 16)]
    return groups + [pair(u, u) + pair(u + 1, u + 1) for u in range(0, 16, 2)]


def mirror_place():
    u, v = lax.axis_index("row") // 2, lax.axis_index("col")
    return jnp.where(u == v, (u % 2) * 2, jnp.where(u < v, 2, 0))


def on_device(ancestor, inverse_first, panel_first, structure_first, inverse_second, panel_second, structure_second):
    panel, near, mixed = kernel(
        lay_body,
        (VMEM, VMEM, VMEM),
        (((32, 16, 128), F32), ((24, 128), F32), ((8, 40, 128), F32)),
        (pltpu.VMEM((128, 128), F32),),
    )(panel_first.transpose(1, 2, 0), panel_second.transpose(1, 2, 0), inverse_first)
    packed, slot1, slot2, table = kernel(
        rank_body,
        (VMEM, VMEM, VMEM),
        (
            ((TALL, 256), F32),
            ((12, 128), jnp.int32),
            ((12, 128), jnp.int32),
            ((384, 256), BF16),
        ),
        (pltpu.VMEM((3 * TALL, 1152), BF16), pltpu.VMEM((1152, 256), BF16), pltpu.VMEM((TALL, 128), F32)),
    )(structure_first.reshape(12, 128), structure_second.reshape(12, 128), ancestor)
    blocks = lax.all_gather(packed, "col")
    mine = exchanged(mixed, "col", Z_GROUPS)
    other = swapped(mine)
    panels = lax.all_to_all(panel, "row", 0, 0, tiled=True)
    (later,) = kernel(list_body, (VMEM,), (((2, 384), jnp.int32),))(structure_second.reshape(12, 128))
    slot1, slot2 = slot1.reshape(1536), slot2.reshape(1536)
    rows = pltpu.VMEM((1536, 128), F32)
    second, fold, extra = kernel(
        second_body,
        (SMEM, VMEM, VMEM, VMEM, VMEM),
        (((1032, 128), F32), ((8, 40, 128), F32), ((32, 128), F32)),
        (rows,),
    )(later, panels, near, mine, other)
    folds = exchanged(fold, "row", Y_GROUPS)
    folds = exchanged(jnp.broadcast_to(folds, (4, *folds.shape)), "row", X_GROUPS)
    (spread,) = kernel(first_body, (SMEM, VMEM), (((EXT + 8, 128), F32),), (rows,))(slot2, panels)
    big = pltpu.VMEM((EXT, 128), F32)
    right, send = kernel(
        image_body,
        (SMEM, VMEM, ANY, ANY, VMEM, VMEM),
        (((EXT, 128), F32), ((4, 64, 128), F32)),
        (rows, pltpu.VMEM((16, TALL, 256), F32), big, big, pltpu.SemaphoreType.DMA((3,))),
        (ANY, VMEM),
    )(slot1, folds, spread, blocks, extra, jnp.asarray(column_choice(), BF16))
    got = exchanged(send, ("row", "col"), mirror_groups())
    whole, share, own = kernel(
        cross_body,
        (VMEM, VMEM, VMEM),
        (((48, 384), F32), ((8, 72, 128), F32), ((16, 128), F32)),
    )(got, jnp.asarray(lane_order(), BF16), table)
    mine = exchanged(share, "col", Z_GROUPS)
    left1, left2 = kernel(pack_body, (VMEM,), (((2, 9, 4, 128), F32), ((1, 9, 4, 128), F32)))(whole)
    other = swapped(mine)
    return kernel(
        diagonal_body,
        (VMEM,) * 9,
        (((2, 11, 4, 128), F32), ((1, 12, 4, 128), F32)),
    )(mine, other, right, second, own, inverse_first, inverse_second, left1, left2)


def solution(mesh):
    tiles = P(None, None, "row", "col")
    panels = P("row", None, "col")

    return jax.shard_map(
        on_device,
        mesh=mesh,
        in_specs=(tiles, tiles, panels, P(), tiles, panels, P()),
        out_specs=(tiles, tiles),
        check_vma=False,
    )
```

```python
import jax
import jax.numpy as jnp
import numpy as np
from jax import lax
from jax.experimental import pallas as pl
from jax.experimental.pallas import tpu as pltpu
from jax.sharding import PartitionSpec as P


F32 = jnp.float32
BF16 = jnp.bfloat16
TALL = 144
SLOTS = 128
EXT = 16 * SLOTS

Y_GROUPS = [[4 * y + x for y in range(8)] for x in range(4)]
X_GROUPS = [[4 * y + x for x in range(4)] for y in range(8)]
Z_GROUPS = [[2 * z + k for z in range(8)] for k in range(2)]


def column_choice():
    table = np.zeros((96, 128), np.float32)
    for h in range(2):
        for m in range(32):
            al, k, q = m // 8, (m % 8) // 4, m % 4
            table[h * 48 + m, k * 32 + h * 16 + 4 * q + al] = 1
        for m in range(16):
            al, q = m // 4, m % 4
            table[h * 48 + 32 + m, 64 + h * 16 + 4 * q + al] = 1
    return table


def lane_order():
    table = np.zeros((512, 512), np.float32)
    for g in range(2):
        for al in range(4):
            for i in range(9):
                for q in range(4):
                    table[g * 256 + i * 16 + al * 4 + q, i * 32 + g * 16 + 4 * q + al] = 1
            for k in range(2):
                for q in range(4):
                    table[g * 256 + TALL + al * 8 + k * 4 + q, 384 + k * 32 + g * 16 + 4 * q + al] = 1
    return table


def dot(left, right):
    return jnp.dot(left, right, preferred_element_type=F32)


def halves(x):
    high = x.astype(BF16)
    return high, (x - high.astype(F32)).astype(BF16)


def thirds(x):
    high = x.astype(BF16)
    rest = x - high.astype(F32)
    mid = rest.astype(BF16)
    return high, mid, (rest - mid.astype(F32)).astype(BF16)


def product_terms(left, right):
    return dot(jnp.concatenate(halves(left), 0), jnp.concatenate(halves(right), 1))


def folded(terms):
    m, n = terms.shape[0] // 2, terms.shape[1] // 2
    return terms[:m, :n] + (terms[:m, n:] + terms[m:, :n])


def chosen(x, table):
    m = x.shape[0]
    out = dot(jnp.concatenate(thirds(x), 0), table)
    return out[:m] + (out[m : 2 * m] + out[2 * m :])


def lanes_of(shape):
    return lax.broadcasted_iota(jnp.int32, shape, len(shape) - 1)


def rank_body(s1, s2, tiles, packed, slot1, slot2, table, lhs, rhs, stage):
    col = lax.axis_index("col")
    upper = (
        lax.broadcasted_iota(jnp.int32, (128, 128), 0) < lax.broadcasted_iota(jnp.int32, (128, 128), 1)
    ).astype(BF16)
    groups = lax.broadcasted_iota(jnp.int32, (16, 128), 0)
    ranks = []
    for which, (source, target) in enumerate(((s1, slot1), (s2, slot2))):
        carry = jnp.zeros((16, 1), F32)
        rank = []
        for m in range(12):
            row = source[m : m + 1, :]
            group = jnp.bitwise_and(lax.shift_right_logical(row, 5), 15)
            inside = row < 4608
            mark = ((group == groups) & inside).astype(F32)
            before = dot(mark.astype(BF16), upper) + carry
            t = jnp.sum(mark * before, axis=0, keepdims=True)
            carry = carry + jnp.sum(mark, axis=1, keepdims=True)
            rank.append(t + 1.0)
            place = group * SLOTS + t.astype(jnp.int32)
            if which:
                place = jnp.where(inside, place, EXT)
            target[m : m + 1, :] = place
        ranks.append(rank)
    slots = lanes_of((32, 128)).astype(F32)
    table[288:, :] = jnp.zeros((96, 256), BF16)
    for j in range(9):
        spots = lax.broadcasted_iota(jnp.int32, (32, 128), 0) + (j * 512 + col * 32)
        both = []
        for source, rank in ((s1, ranks[0]), (s2, ranks[1])):
            total = jnp.zeros((32, 128), F32)
            for m in range(12):
                total = total + jnp.where(source[m : m + 1, :] == spots, rank[m], 0.0)
            slot = jnp.sum(total, axis=1, keepdims=True) - 1.0
            both.append((slot == slots).astype(BF16))
        pair = jnp.concatenate(both, 1)
        table[j * 32 : (j + 1) * 32, :] = pair
        for al in range(4):
            rhs[j * 128 + al * 32 : j * 128 + (al + 1) * 32, :] = pair
        quarter = lanes_of((4, 128)) // 32
        for i in range(9):
            for al in range(4):
                stage[i * 16 + al * 4 : i * 16 + (al + 1) * 4, :] = jnp.where(quarter == al, tiles[i, j], 0.0)
        for part, value in enumerate(thirds(stage[...])):
            lhs[part * TALL : (part + 1) * TALL, j * 128 : (j + 1) * 128] = value
    out = dot(lhs[...], rhs[...])
    packed[...] = out[:TALL] + (out[TALL : 2 * TALL] + out[2 * TALL :])


def list_body(s2, later):
    upper = (
        lax.broadcasted_iota(jnp.int32, (128, 128), 0) < lax.broadcasted_iota(jnp.int32, (128, 128), 1)
    ).astype(BF16)
    row = s2[...]
    group = jnp.bitwise_and(lax.shift_right_logical(row, 5), 15)
    high = lax.shift_right_logical(row - 4608, 9)
    other = group * 64 + high * 32 + jnp.bitwise_and(row, 31)
    mark = jnp.where(row < 4608, 0.0, 1.0)
    order = dot(jnp.concatenate([mark, mark[:4]], 0).astype(BF16), upper)[:12]
    total = jnp.sum(mark, axis=1, keepdims=True)
    count = jnp.zeros((1, 1), F32)
    spot = lax.broadcasted_iota(jnp.int32, (384, 128), 0).astype(F32)
    kind = lax.broadcasted_iota(jnp.int32, (8, 128), 0)
    matches, values = [], []
    for m in range(12):
        place = jnp.where(mark[m : m + 1] > 0, order[m : m + 1] + count, -1.0)
        count = count + total[m : m + 1]
        index = lanes_of((1, 128)) + m * 128
        value = jnp.where(kind == 0, lax.shift_right_logical(index, 6), jnp.bitwise_and(index, 63))
        value = jnp.where(kind == 2, lax.shift_right_logical(other[m : m + 1], 6), value)
        value = jnp.where(kind == 3, jnp.bitwise_and(other[m : m + 1], 63), value)
        values.append(jnp.where(kind == 4, 1, value).astype(F32).astype(BF16))
        matches.append((place == spot).astype(BF16))
    listed = lax.dot_general(
        jnp.concatenate(values, 1),
        jnp.concatenate(matches, 1),
        (((1,), (1,)), ((), ())),
        preferred_element_type=F32,
    )
    source_row = listed[0:1] * 64.0 + listed[1:2]
    target_row = jnp.where(listed[4:5] > 0.5, listed[2:3] * 64.0 + listed[3:4], 1024.0)
    later[...] = jnp.concatenate([source_row, target_row], 0).astype(jnp.int32)


def lay_body(p1, p2, d1, panel, near, mixed, tall):
    tall[...] = jnp.zeros((128, 128), F32)
    tall[0:32, 0:48] = p1[0]
    tall[32:64, 0:48] = p1[1]
    tall[64:96, 0:48] = p2[0]
    both = tall[...].T[:48]
    lane = lanes_of((16, 128))
    value = jnp.zeros((16, 128), F32)
    for h in range(3):
        moved = pltpu.roll(both[16 * h : 16 * (h + 1)], (32 * h - 64) % 128, 1)
        value = jnp.where(lane // 32 == h, moved, value)
    for n in range(32):
        panel[n] = value
    near[...] = jnp.where(lanes_of((24, 128)) < 64, both[:24], pltpu.roll(both[24:], 64, 1))
    lane = lanes_of((4, 128))
    tall[0:48, :] = both
    for al in range(4):
        for k in range(2):
            value = jnp.zeros((4, 128), F32)
            for m in range(2):
                value = jnp.where(lane // 32 == m, pltpu.roll(d1[k, m], ((m - al) * 32) % 128, 1), value)
            tall[48 + al * 8 + k * 4 : 52 + al * 8 + k * 4, :] = value
    half = lanes_of((40, 128)) < 64
    value = jnp.where(half, tall[0:40, :], pltpu.roll(tall[40:80, :], 64, 1))
    for n in range(8):
        mixed[n] = value


def scatter_rows(slots, source, target):
    def place(step, _):
        base = pl.multiple_of(step * 96, 32)
        for u in range(96):
            target[pl.ds(slots[base + u], 1), :] = source[pl.ds(base + u, 1), :]
        return 0

    lax.fori_loop(0, 16, place, 0)


def in_order(step):
    return ((step % 8) * 4 + step // 8) * 48


def unfold(folds, rows, low):
    keep = lanes_of((16, 128))
    keep = (keep >= low) & (keep < low + 32)
    for r in range(32):
        for h in range(3):
            moved = pltpu.roll(folds[r], (low - 32 * h) % 128, 1)
            rows[r * 48 + 16 * h : r * 48 + 16 * (h + 1), :] = jnp.where(keep, moved, 0.0)


def second_body(later, panels, near, mine, other, spread, fold, extra, rows):
    unfold(panels, rows, 64)
    spread[...] = jnp.zeros(spread.shape, F32)

    def place(step, _):
        for u in range(48):
            n = step * 48 + u
            spread[pl.ds(later[1, n], 1), :] = rows[pl.ds(later[0, n], 1), :]
        return 0

    lax.fori_loop(0, 8, place, 0)
    core = lax.axis_index("col") % 2
    half = lanes_of((40, 128)) < 64
    total = jnp.zeros((160, 256), F32)
    for z in range(8):
        left, right = [], []
        for source, k in ((mine, core), (other, 1 - core)):
            x = source[z]
            left.append(jnp.concatenate([jnp.where(half, x, 0.0), jnp.where(half, 0.0, x)], 0))
            right += 2 * [spread[pl.ds(pl.multiple_of((2 * z + k) * 64, 64), 64), :]]
        total = total + product_terms(jnp.concatenate(left, 1), jnp.concatenate(right, 0))
    out = folded(total)
    lane_f = lanes_of((16, 128))
    value = jnp.zeros((16, 128), F32)
    for h in range(3):
        moved = pltpu.roll(out[16 * h : 16 * (h + 1), :], (32 * h - 64) % 128, 1)
        value = jnp.where(lane_f // 32 == h, moved, value)
    value = jnp.concatenate([value, near[...]], 0)
    for n in range(8):
        fold[n] = value
    extra[...] = out[48:80, :]


def first_body(slot2, panels, spread, rows):
    unfold(panels, rows, 96)
    spread[...] = jnp.zeros(spread.shape, F32)
    scatter_rows(slot2, rows, spread)


def image_body(slot1, folds, second_hbm, blocks, extra, choice, out, send, rows, held, second, right, done):
    third = pltpu.make_async_copy(second_hbm.at[pl.ds(0, EXT)], second, done.at[0])
    arrival = pltpu.make_async_copy(blocks, held, done.at[1])
    leaving = pltpu.make_async_copy(right, out, done.at[2])
    third.start()
    arrival.start()
    lane = lanes_of((16, 128))
    for step in range(32):
        piece = folds[step // 8, step % 8]
        base = in_order(step)
        near = jnp.concatenate([piece[16:], pltpu.roll(piece[16:], 64, 1)], 0)
        for h in range(3):
            moved = jnp.where(lane < 96, -pltpu.roll(piece[:16], (64 - 32 * h) % 128, 1), 0.0)
            rows[base + 16 * h : base + 16 * (h + 1), :] = jnp.where(lane < 64, near[16 * h : 16 * (h + 1)], moved)
    right[...] = jnp.zeros(right.shape, F32)
    scatter_rows(slot1, rows, right)
    third.wait()
    right[...] = right[...] + second[...]
    leaving.start()
    arrival.wait()
    total = jnp.zeros((4 * TALL, 256), F32)
    for c in range(0, 16, 2):
        left = [jnp.concatenate([held[c, :, n : n + 128], held[c + 1, :, n : n + 128]], 1) for n in (0, 128)]
        total = total + product_terms(jnp.concatenate(left, 0), right[c * SLOTS : (c + 2) * SLOTS, :])
    out_terms = folded(total)
    image = out_terms[:TALL]
    late = lanes_of((TALL, 128))
    image = jnp.where((late >= 64) & (late < 96), image + pltpu.roll(out_terms[TALL:], 96, 1), image)
    image = jnp.concatenate([image, extra[...]], 0)
    sent = jnp.zeros((96, TALL + 32), F32)
    for part in thirds(image):
        sent = sent + lax.dot_general(choice[...], part, (((1,), (1,)), ((), ())), preferred_element_type=F32)
    lane = lanes_of((16, 128))
    pieces = []
    for h in range(2):
        rest = jnp.concatenate([sent[h * 48 : (h + 1) * 48, 128:], jnp.zeros((48, 80), F32)], 1)
        tail = jnp.where(lane < 16, rest[0:16], pltpu.roll(rest[16:32], 16, 1))
        tail = jnp.where(lane < 32, tail, pltpu.roll(rest[32:48], 32, 1))
        pieces.append(jnp.concatenate([sent[h * 48 : (h + 1) * 48, :128], tail], 0))
    place = mirror_place()
    send[...] = jnp.zeros(send.shape, F32)
    for h in range(2):
        send[pl.ds(place + h, 1)] = pieces[h][None]
    leaving.wait()


def cross_body(got, order, table, whole, share, own):
    place = mirror_place()
    parts = []
    for g in range(2):
        piece = got[pl.ds(place + g, 1)][0]
        tail = piece[48:64]
        parts.append(piece[:48])
        parts.append(jnp.concatenate([tail, pltpu.roll(tail, 112, 1), pltpu.roll(tail, 96, 1)], 0))
    y = chosen(jnp.concatenate(parts, 1), order[...])
    close = chosen(y[:, :384], table[...])
    e = y[32:48, 384:512]
    own[...] = e
    lane = lanes_of((8, 128))
    e = jnp.where(lane < 64, e[:8], pltpu.roll(e[8:], 64, 1))
    e = jnp.concatenate([close[:, :128], close[32:48, 128:], e], 0)
    for n in range(8):
        share[n] = e
    whole[...] = y[:, :384]


def pack_body(whole, first, second):
    y = whole[...]
    lane = lanes_of((8, 128))
    lane2 = lanes_of((4, 128))
    for i in range(9):
        chunk = (i // 4) * 128
        one = jnp.zeros((8, 128), F32)
        two = jnp.zeros((4, 128), F32)
        for al in range(4):
            shift = ((al - i % 4) * 32) % 128
            moved = pltpu.roll(y[al * 8 : (al + 1) * 8, chunk : chunk + 128], shift, 1) if shift else y[al * 8 : (al + 1) * 8, chunk : chunk + 128]
            one = jnp.where(lane // 32 == al, moved, one)
            low = y[32 + al * 4 : 36 + al * 4, chunk : chunk + 128]
            moved = pltpu.roll(low, shift, 1) if shift else low
            two = jnp.where(lane2 // 32 == al, moved, two)
        first[0, i] = -one[0:4]
        first[1, i] = -one[4:8]
        second[0, i] = -two


def diagonal_body(mine, other, right, later, own, d1, d2, left1, left2, first, second):
    first[:, 0:9] = left1[...]
    second[:, 0:9] = left2[...]
    core = lax.axis_index("col") % 2
    lane_e = lanes_of((8, 128))
    total = jnp.zeros((128, 256), F32)
    also = jnp.zeros((32, 256), F32)
    for z in range(8):
        left, wide, extra, late = [], [], [], []
        for source, k in ((mine, core), (other, 1 - core)):
            c = 2 * z + k
            x = source[z]
            left.append(x[:64])
            wide.append(right[pl.ds(pl.multiple_of(c * SLOTS, SLOTS), SLOTS), :])
            e = x[64:72]
            extra.append(jnp.concatenate([jnp.where(lane_e < 64, e, 0.0), jnp.where(lane_e >= 64, e, 0.0)], 0))
            late += 2 * [later[pl.ds(pl.multiple_of(c * 64, 64), 64), :]]
        total = total + product_terms(jnp.concatenate(left, 1), jnp.concatenate(wide, 0))
        also = also + product_terms(jnp.concatenate(extra, 1), jnp.concatenate(late, 0))
    out = folded(total)
    g1 = out[:32]
    bottom = own[...] - out[32:48]
    g2 = out[32:48] + pltpu.roll(out[48:64], 96, 1) + folded(also)
    lane = lanes_of((8, 128))
    lane2 = lanes_of((4, 128))
    for k in range(2):
        one = jnp.zeros((8, 128), F32)
        two = jnp.zeros((4, 128), F32)
        for al in range(4):
            shift = ((al - k) * 32) % 128
            one = jnp.where(lane // 32 == al, pltpu.roll(g1[al * 8 : (al + 1) * 8], shift, 1), one)
            two = jnp.where(lane2 // 32 == al, pltpu.roll(bottom[al * 4 : (al + 1) * 4], shift, 1), two)
        first[0, 9 + k] = d1[0, k] + one[0:4]
        first[1, 9 + k] = d1[1, k] + one[4:8]
        second[0, 9 + k] = -two
    two = jnp.zeros((4, 128), F32)
    for al in range(4):
        shift = ((al - 2) * 32) % 128
        two = jnp.where(lane2 // 32 == al, pltpu.roll(g2[al * 4 : (al + 1) * 4], shift, 1), two)
    second[0, 11] = d2[0, 0] + two


VMEM = pl.BlockSpec(memory_space=pltpu.VMEM)
SMEM = pl.BlockSpec(memory_space=pltpu.SMEM)
ANY = pl.BlockSpec(memory_space=pl.ANY)


def kernel(body, specs, outs, scratch=(), places=None):
    return pl.pallas_call(
        body,
        in_specs=list(specs),
        out_specs=list(places or [VMEM] * len(outs)),
        out_shape=[jax.ShapeDtypeStruct(shape, dtype) for shape, dtype in outs],
        scratch_shapes=list(scratch),
    )


def exchanged(x, axis, groups):
    return lax.all_to_all(x, axis, 0, 0, axis_index_groups=groups, tiled=True)


def swapped(x):
    return lax.ppermute(x, "col", [(c, c ^ 1) for c in range(16)])


def mirror_groups():
    def pair(u, v):
        return [(2 * u) * 16 + v, (2 * u + 1) * 16 + v]

    groups = [pair(u, v) + pair(v, u) for u in range(16) for v in range(u + 1, 16)]
    return groups + [pair(u, u) + pair(u + 1, u + 1) for u in range(0, 16, 2)]


def mirror_place():
    u, v = lax.axis_index("row") // 2, lax.axis_index("col")
    return jnp.where(u == v, (u % 2) * 2, jnp.where(u < v, 2, 0))


def on_device(ancestor, inverse_first, panel_first, structure_first, inverse_second, panel_second, structure_second):
    panel, near, mixed = kernel(
        lay_body,
        (VMEM, VMEM, VMEM),
        (((32, 16, 128), F32), ((24, 128), F32), ((8, 40, 128), F32)),
        (pltpu.VMEM((128, 128), F32),),
    )(panel_first.transpose(1, 2, 0), panel_second.transpose(1, 2, 0), inverse_first)
    packed, slot1, slot2, table = kernel(
        rank_body,
        (VMEM, VMEM, VMEM),
        (
            ((TALL, 256), F32),
            ((12, 128), jnp.int32),
            ((12, 128), jnp.int32),
            ((384, 256), BF16),
        ),
        (pltpu.VMEM((3 * TALL, 1152), BF16), pltpu.VMEM((1152, 256), BF16), pltpu.VMEM((TALL, 128), F32)),
    )(structure_first.reshape(12, 128), structure_second.reshape(12, 128), ancestor)
    blocks = lax.all_gather(packed, "col")
    mine = exchanged(mixed, "col", Z_GROUPS)
    other = swapped(mine)
    panels = lax.all_to_all(panel, "row", 0, 0, tiled=True)
    (later,) = kernel(list_body, (VMEM,), (((2, 384), jnp.int32),))(structure_second.reshape(12, 128))
    slot1, slot2 = slot1.reshape(1536), slot2.reshape(1536)
    rows = pltpu.VMEM((1536, 128), F32)
    second, fold, extra = kernel(
        second_body,
        (SMEM, VMEM, VMEM, VMEM, VMEM),
        (((1032, 128), F32), ((8, 40, 128), F32), ((32, 128), F32)),
        (rows,),
    )(later, panels, near, mine, other)
    folds = exchanged(fold, "row", Y_GROUPS)
    folds = exchanged(jnp.broadcast_to(folds, (4, *folds.shape)), "row", X_GROUPS)
    (spread,) = kernel(first_body, (SMEM, VMEM), (((EXT + 8, 128), F32),), (rows,))(slot2, panels)
    big = pltpu.VMEM((EXT, 128), F32)
    right, send = kernel(
        image_body,
        (SMEM, VMEM, ANY, ANY, VMEM, VMEM),
        (((EXT, 128), F32), ((4, 64, 128), F32)),
        (rows, pltpu.VMEM((16, TALL, 256), F32), big, big, pltpu.SemaphoreType.DMA((3,))),
        (ANY, VMEM),
    )(slot1, folds, spread, blocks, extra, jnp.asarray(column_choice(), BF16))
    got = exchanged(send, ("row", "col"), mirror_groups())
    whole, share, own = kernel(
        cross_body,
        (VMEM, VMEM, VMEM),
        (((48, 384), F32), ((8, 72, 128), F32), ((16, 128), F32)),
    )(got, jnp.asarray(lane_order(), BF16), table)
    mine = exchanged(share, "col", Z_GROUPS)
    left1, left2 = kernel(pack_body, (VMEM,), (((2, 9, 4, 128), F32), ((1, 9, 4, 128), F32)))(whole)
    other = swapped(mine)
    return kernel(
        diagonal_body,
        (VMEM,) * 9,
        (((2, 11, 4, 128), F32), ((1, 12, 4, 128), F32)),
    )(mine, other, right, second, own, inverse_first, inverse_second, left1, left2)


def solution(mesh):
    tiles = P(None, None, "row", "col")
    panels = P("row", None, "col")

    return jax.shard_map(
        on_device,
        mesh=mesh,
        in_specs=(tiles, tiles, panels, P(), tiles, panels, P()),
        out_specs=(tiles, tiles),
        check_vma=False,
    )
```
